16 devices in a mesh: fsdp: 16 (over z, y, x, core).
Axes of the slice: x: 2, y: 2, z: 2, core: 2. Of those that a mesh axis runs over, the one named last changes fastest.
Arguments:
- hidden: bfloat16 [16, 512, 1536], P('fsdp')
- grad_out: bfloat16 [16, 512, 1536], P('fsdp')
- positions: int32 [16, 512], P('fsdp')
- gain_attn: bfloat16 [1536], P('fsdp')
- w_q: bfloat16 [1536, 1536], P('fsdp')
- b_q: bfloat16 [1536], P('fsdp')
- w_k: bfloat16 [1536, 256], P('fsdp')
- b_k: bfloat16 [256], P('fsdp')
- w_v: bfloat16 [1536, 256], P('fsdp')
- b_v: bfloat16 [256], P('fsdp')
- w_o: bfloat16 [1536, 1536], P('fsdp')
- gain_mlp: bfloat16 [1536], P('fsdp')
- w_gate: bfloat16 [1536, 8960], P('fsdp')
- w_up: bfloat16 [1536, 8960], P('fsdp')
- w_down: bfloat16 [8960, 1536], P('fsdp')
Outputs:
- output 1: bfloat16 [16, 512, 1536], P('fsdp')
- output 2: bfloat16 [16, 512, 1536], P('fsdp')
- output 3: float32 [1536], P('fsdp')
- output 4: float32 [1536, 1536], P('fsdp')
- output 5: float32 [1536], P('fsdp')
- output 6: float32 [1536, 256], P('fsdp')
- output 7: float32 [256], P('fsdp')
- output 8: float32 [1536, 256], P('fsdp')
- output 9: float32 [256], P('fsdp')
- output 10: float32 [1536, 1536], P('fsdp')
- output 11: float32 [1536], P('fsdp')
- output 12: float32 [1536, 8960], P('fsdp')
- output 13: float32 [1536, 8960], P('fsdp')
- output 14: float32 [8960, 1536], P('fsdp')
All inputs are finite; a program needn't handle non-finite values.
Results may differ from the reference program's by a relative error of at most 0.0171064.
Values are sent between devices in bfloat16 or wider.
A program may use at most 1 GiB of HBM per device.

```python
import math
import jax
import jax.numpy as jnp
from jax import lax

D = 1536
HEADS = 12
KV_HEADS = 2
HEAD = 128
FF = 8960
BATCH = 16
SEQ = 512
NORM_EPS = 1e-6
ROPE_THETA = 1000000.0
GROUP_SEQS = math.gcd(BATCH, max(1, 512 // SEQ))


def setup_inputs(seed: int = 0) -> dict:
    key_list = jax.random.split(jax.random.key(seed), 16)
    q_width = HEADS * HEAD
    kv_width = KV_HEADS * HEAD
    scale_d = 1.0 / math.sqrt(D)

    def normal_f32(key_index, arr_shape):
        return jax.random.normal(key_list[key_index], arr_shape, jnp.float32)

    pos_gaps = jax.random.randint(key_list[2], (BATCH, SEQ), 1, 9)
    pos_starts = jax.random.randint(key_list[3], (BATCH, 1), 0, 512)
    positions = (pos_starts + jnp.cumsum(pos_gaps, axis=1) - 1).astype(jnp.int32)
    return {
        'hidden': normal_f32(0, (BATCH, SEQ, D)).astype(jnp.bfloat16),
        'grad_out': normal_f32(1, (BATCH, SEQ, D)).astype(jnp.bfloat16),
        'positions': positions,
        'gain_attn': (1.0 + 0.3 * normal_f32(4, (D,))).astype(jnp.bfloat16),
        'w_q': (normal_f32(5, (D, q_width)) * scale_d).astype(jnp.bfloat16),
        'b_q': (0.5 * normal_f32(6, (q_width,))).astype(jnp.bfloat16),
        'w_k': (normal_f32(7, (D, kv_width)) * scale_d).astype(jnp.bfloat16),
        'b_k': normal_f32(8, (kv_width,)).astype(jnp.bfloat16),
        'w_v': (normal_f32(9, (D, kv_width)) * scale_d).astype(jnp.bfloat16),
        'b_v': (0.5 * normal_f32(10, (kv_width,))).astype(jnp.bfloat16),
        'w_o': (normal_f32(11, (q_width, D)) / math.sqrt(q_width)).astype(jnp.bfloat16),
        'gain_mlp': (1.0 + 0.3 * normal_f32(12, (D,))).astype(jnp.bfloat16),
        'w_gate': (normal_f32(13, (D, FF)) * scale_d).astype(jnp.bfloat16),
        'w_up': (normal_f32(14, (D, FF)) * scale_d).astype(jnp.bfloat16),
        'w_down': (normal_f32(15, (FF, D)) / math.sqrt(FF)).astype(jnp.bfloat16),
    }


def rope_tables(positions):
    inv_freq = 1.0 / jnp.power(ROPE_THETA, jnp.arange(0, HEAD, 2).astype(jnp.float32) / HEAD)
    angles = positions.astype(jnp.float32)[:, :, None] * inv_freq
    angles = jnp.concatenate([angles, angles], axis=-1)[:, :, None, :]
    return jnp.cos(angles), jnp.sin(angles)


def rotate_half(vec_in):
    half_dim = vec_in.shape[-1] // 2
    return jnp.concatenate([-vec_in[..., half_dim:], vec_in[..., :half_dim]], axis=-1)


def rms_norm(val_f32, gain_vec):
    inv_rms = lax.rsqrt(jnp.mean(val_f32 * val_f32, axis=-1, keepdims=True) + NORM_EPS)
    return (val_f32 * inv_rms * gain_vec).astype(jnp.bfloat16).astype(jnp.float32)


def layer_forward(params, hidden, positions):
    gain_attn, w_q, b_q, w_k, b_k, w_v, b_v, w_o, gain_mlp, w_gate, w_up, w_down = params
    n_batch = hidden.shape[0]
    q_per_kv = HEADS // KV_HEADS
    cos_t, sin_t = rope_tables(positions)
    hidden_f32 = hidden.astype(jnp.float32)
    normed_attn = rms_norm(hidden_f32, gain_attn)
    q_lin = (jnp.einsum('bsd,de->bse', normed_attn, w_q) + b_q).reshape(n_batch, SEQ, HEADS, HEAD)
    k_lin = (jnp.einsum('bsd,de->bse', normed_attn, w_k) + b_k).reshape(n_batch, SEQ, KV_HEADS, HEAD)
    v_states = (jnp.einsum('bsd,de->bse', normed_attn, w_v) + b_v).astype(jnp.bfloat16).astype(jnp.float32)
    v_states = v_states.reshape(n_batch, SEQ, KV_HEADS, HEAD)
    q_states = (q_lin * cos_t + rotate_half(q_lin) * sin_t).astype(jnp.bfloat16).astype(jnp.float32)
    q_states = q_states.reshape(n_batch, SEQ, KV_HEADS, q_per_kv, HEAD)
    k_states = (k_lin * cos_t + rotate_half(k_lin) * sin_t).astype(jnp.bfloat16).astype(jnp.float32)
    scores = jnp.einsum('bqkgd,bskd->bkgqs', q_states, k_states) / math.sqrt(HEAD)
    causal = jnp.arange(SEQ)[:, None] >= jnp.arange(SEQ)[None, :]
    attn_probs = jax.nn.softmax(jnp.where(causal, scores, -1e30), axis=-1)
    attn_probs = attn_probs.astype(jnp.bfloat16).astype(jnp.float32)
    attn_out = jnp.einsum('bkgqs,bskd->bqkgd', attn_probs, v_states).astype(jnp.bfloat16).astype(jnp.float32)
    attn_out = attn_out.reshape(n_batch, SEQ, HEADS * HEAD)
    resid_mid = (hidden_f32 + jnp.einsum('bse,ed->bsd', attn_out, w_o)).astype(jnp.bfloat16).astype(jnp.float32)
    normed_mlp = rms_norm(resid_mid, gain_mlp)
    gate_pre = jnp.einsum('bsd,df->bsf', normed_mlp, w_gate)
    up_proj = jnp.einsum('bsd,df->bsf', normed_mlp, w_up)
    act_mlp = (jax.nn.silu(gate_pre) * up_proj).astype(jnp.bfloat16).astype(jnp.float32)
    return (resid_mid + jnp.einsum('bsf,fd->bsd', act_mlp, w_down)).astype(jnp.bfloat16)


def reference(hidden, grad_out, positions, gain_attn, w_q, b_q, w_k, b_k, w_v, b_v, w_o, gain_mlp, w_gate, w_up, w_down):
    params = tuple(weight_arr.astype(jnp.float32) for weight_arr in (gain_attn, w_q, b_q, w_k, b_k, w_v, b_v, w_o, gain_mlp, w_gate, w_up, w_down))
    n_steps = BATCH // GROUP_SEQS

    def scan_body(grad_acc, step_in):
        hid_step, gout_step, pos_step = step_in

        def forward_only(param_list, hid_in):
            return layer_forward(param_list, hid_in, pos_step)

        layer_out, pullback = jax.vjp(forward_only, params, hid_step)
        d_params, d_hidden = pullback(gout_step)
        return jax.tree.map(jnp.add, grad_acc, d_params), (layer_out, d_hidden)

    step_inputs = (
        hidden.reshape(n_steps, GROUP_SEQS, SEQ, D),
        grad_out.reshape(n_steps, GROUP_SEQS, SEQ, D),
        positions.reshape(n_steps, GROUP_SEQS, SEQ),
    )
    grad_init = jax.tree.map(jnp.zeros_like, params)
    grad_sum, (out_steps, dx_steps) = lax.scan(scan_body, grad_init, step_inputs)
    return (out_steps.reshape(BATCH, SEQ, D), dx_steps.reshape(BATCH, SEQ, D), grad_sum[0], grad_sum[1], grad_sum[2], grad_sum[3], grad_sum[4], grad_sum[5], grad_sum[6], grad_sum[7], grad_sum[8], grad_sum[9], grad_sum[10], grad_sum[11])
```

```python
import math
import jax
import jax.numpy as jnp
from jax import lax
from jax.sharding import PartitionSpec as P

HEAD_DIM = 128
NORM_EPS = 1e-6
ROPE_THETA = 1000000.0
AX = 'fsdp'
N_DEV = 16
TP = 8
GROUPS = [list(range(0, 8)), list(range(8, 16))]
Z_PERM = [(i, i ^ 8) for i in range(N_DEV)]
F32 = jnp.float32
BF16 = jnp.bfloat16


def dot(eq_form, lhs_arr, rhs_arr):
    return jnp.einsum(eq_form, lhs_arr, rhs_arr, preferred_element_type=F32)


def rope_tables(positions):
    inv_freq = 1.0 / jnp.power(ROPE_THETA, jnp.arange(0, HEAD_DIM, 2).astype(F32) / HEAD_DIM)
    angles = positions.astype(F32)[:, None] * inv_freq
    angles = jnp.concatenate([angles, angles], axis=-1)[:, None, :]
    return jnp.cos(angles), jnp.sin(angles)


def rotate_half(vec_in):
    half_dim = vec_in.shape[-1] // 2
    return jnp.concatenate([-vec_in[..., half_dim:], vec_in[..., :half_dim]], axis=-1)


def rotate_half_t(vec_in):
    half_dim = vec_in.shape[-1] // 2
    return jnp.concatenate([vec_in[..., half_dim:], -vec_in[..., :half_dim]], axis=-1)


def norm_fwd(hidden, gain_vec):
    x_f32 = hidden.astype(F32)
    inv_rms = lax.rsqrt(jnp.mean(x_f32 * x_f32, axis=-1, keepdims=True) + NORM_EPS)
    return (x_f32 * inv_rms * gain_vec).astype(BF16), inv_rms


def norm_bwd(hidden, inv_rms, gain_vec, d_normed):
    unit_rows = hidden.astype(F32) * inv_rms
    d_gain = jnp.sum(d_normed * unit_rows, axis=0)
    d_unit = d_normed * gain_vec
    d_hidden = inv_rms * (d_unit - unit_rows * jnp.mean(d_unit * unit_rows, axis=-1, keepdims=True))
    return d_hidden, d_gain


def z_pair(arr):
    return lax.ppermute(arr, AX, Z_PERM)


def local_step(hidden, grad_out, positions, gain_attn, w_q, b_q, w_k, b_k, w_v, b_v, w_o, gain_mlp, w_gate, w_up, w_down):
    n_seq, width = hidden.shape[1], hidden.shape[2]
    rows = w_q.shape[0]
    q_width, kv_width = w_q.shape[1], w_k.shape[1]
    n_heads, n_kv = q_width // HEAD_DIM, kv_width // HEAD_DIM
    q_per_kv = n_heads // n_kv
    ff_blk = w_down.shape[0]
    ff_loc = 2 * ff_blk
    half = width // 2
    n_tok = n_seq
    z_idx = lax.axis_index(AX) // TP
    z_zero = z_idx == 0
    hidden = hidden[0]
    grad_out = grad_out[0]

    kvb = jnp.concatenate([b_k, b_v, jnp.zeros((rows - 2 * b_k.shape[0],), BF16)])
    small = jnp.stack([gain_attn, b_q, gain_mlp, kvb], axis=1)
    small = jnp.pad(small, ((0, 0), (0, 124)))
    qkv_loc = jnp.concatenate([w_q, w_k, w_v, small], axis=1)
    qkv_full = lax.all_gather(qkv_loc, AX, axis=0, tiled=True)
    n_qkv = q_width + 2 * kv_width
    w_qkv = qkv_full[:, :n_qkv]
    small_t = qkv_full[:, n_qkv:n_qkv + 4].T.astype(F32)
    gain_a, bias_q, gain_m = small_t[0], small_t[1], small_t[2]
    kvb_full = small_t[3].reshape(N_DEV, rows)
    n_b = b_k.shape[0]
    bias_k = kvb_full[:, :n_b].reshape(kv_width)
    bias_v = kvb_full[:, n_b:2 * n_b].reshape(kv_width)
    bias = jnp.concatenate([bias_q, bias_k, bias_v])
    w_o_full = lax.all_gather(w_o, AX, axis=0, tiled=True)

    gu = jnp.stack([w_gate, w_up], axis=0).reshape(2, rows, 2, TP, ff_blk)
    gu = gu.transpose(3, 0, 1, 2, 4).reshape(TP, 2 * rows, ff_loc)
    gu = lax.all_to_all(gu, AX, 0, 0, axis_index_groups=GROUPS, tiled=True)
    gu = gu.reshape(TP, 2, rows, ff_loc).transpose(1, 0, 2, 3).reshape(2, half, ff_loc)
    gu_other = z_pair(gu)
    gu_lo = jnp.where(z_zero, gu, gu_other)
    gu_hi = jnp.where(z_zero, gu_other, gu)
    w_g = jnp.concatenate([gu_lo[0], gu_hi[0]], axis=0)
    w_u = jnp.concatenate([gu_lo[1], gu_hi[1]], axis=0)
    down_other = z_pair(w_down)
    w_d = jnp.concatenate([jnp.where(z_zero, w_down, down_other), jnp.where(z_zero, down_other, w_down)], axis=0)

    go_all = lax.all_gather(grad_out, AX, axis=0, tiled=True, axis_index_groups=GROUPS)

    cos_t, sin_t = rope_tables(positions[0])
    normed_attn, inv_attn = norm_fwd(hidden, gain_a)
    qkv = dot('sd,de->se', normed_attn, w_qkv) + bias
    q_lin = qkv[:, :q_width].reshape(n_seq, n_heads, HEAD_DIM)
    k_lin = qkv[:, q_width:q_width + kv_width].reshape(n_seq, n_kv, HEAD_DIM)
    v_states = qkv[:, q_width + kv_width:].astype(BF16).reshape(n_seq, n_kv, HEAD_DIM)
    q_states = (q_lin * cos_t + rotate_half(q_lin) * sin_t).astype(BF16).reshape(n_seq, n_kv, q_per_kv, HEAD_DIM)
    k_states = (k_lin * cos_t + rotate_half(k_lin) * sin_t).astype(BF16)
    scores = dot('qkgd,skd->kgqs', q_states, k_states) / math.sqrt(HEAD_DIM)
    causal = lax.broadcasted_iota(jnp.int32, (n_seq, n_seq), 0) >= lax.broadcasted_iota(jnp.int32, (n_seq, n_seq), 1)
    attn_probs = jax.nn.softmax(jnp.where(causal, scores, -1e30), axis=-1)
    attn_out = dot('kgqs,skd->qkgd', attn_probs.astype(BF16), v_states).astype(BF16).reshape(n_seq, q_width)
    resid_mid = (hidden.astype(F32) + dot('se,ed->sd', attn_out, w_o_full)).astype(BF16)
    normed_mlp, inv_mlp = norm_fwd(resid_mid, gain_m)

    h_all = lax.all_gather(normed_mlp, AX, axis=0, tiled=True, axis_index_groups=GROUPS)
    gate_pre = dot('sd,df->sf', h_all, w_g)
    up_proj = dot('sd,df->sf', h_all, w_u)
    act = (jax.nn.silu(gate_pre) * up_proj).astype(BF16)
    d_act = dot('sd,fd->sf', go_all, w_d).astype(BF16).astype(F32)
    gate_sig = jax.nn.sigmoid(gate_pre)
    d_gate = (d_act * up_proj * gate_sig * (1.0 + gate_pre * (1.0 - gate_sig))).astype(BF16)
    d_up = (d_act * gate_pre * gate_sig).astype(BF16)
    dn_part = dot('sf,df->sd', d_gate, w_g) + dot('sf,df->sd', d_up, w_u)
    d_normed_mlp = lax.psum_scatter(dn_part, AX, scatter_dimension=0, tiled=True, axis_index_groups=GROUPS)
    d_normed_mlp = d_normed_mlp.astype(BF16).astype(F32)

    out_part = dot('sf,fd->sd', act, w_d)
    out_sum = lax.psum_scatter(out_part, AX, scatter_dimension=0, tiled=True, axis_index_groups=GROUPS)
    layer_out = (resid_mid.astype(F32) + out_sum).astype(BF16)

    d_wd = dot('sf,sd->fd', act, go_all)
    d_wd_send = lax.dynamic_slice_in_dim(d_wd, (1 - z_idx) * ff_blk, ff_blk, axis=0)
    d_wd_keep = lax.dynamic_slice_in_dim(d_wd, z_idx * ff_blk, ff_blk, axis=0)
    g_w_down = d_wd_keep + z_pair(d_wd_send)
    h_send = lax.dynamic_slice_in_dim(h_all, (1 - z_idx) * half, half, axis=1)
    h_keep = lax.dynamic_slice_in_dim(h_all, z_idx * half, half, axis=1)
    g_g = dot('sd,sf->df', h_keep, d_gate) + z_pair(dot('sd,sf->df', h_send, d_gate))
    g_u = dot('sd,sf->df', h_keep, d_up) + z_pair(dot('sd,sf->df', h_send, d_up))

    def back_rows(grad):
        grad = lax.all_to_all(grad.reshape(TP, rows, ff_loc), AX, 0, 0, axis_index_groups=GROUPS, tiled=True)
        return grad.reshape(TP, rows, 2, ff_blk).transpose(1, 2, 0, 3).reshape(rows, N_DEV * ff_blk)

    g_w_gate = back_rows(g_g)
    g_w_up = back_rows(g_u)

    d_resid_norm, d_gain_m = norm_bwd(resid_mid, inv_mlp, gain_m, d_normed_mlp)
    d_resid = (grad_out.astype(F32) + d_resid_norm).astype(BF16)
    d_w_o = dot('se,sd->ed', attn_out, d_resid)
    d_attn = dot('sd,ed->se', d_resid, w_o_full).astype(BF16).reshape(n_seq, n_kv, q_per_kv, HEAD_DIM)
    d_v_states = dot('kgqs,qkgd->skd', attn_probs.astype(BF16), d_attn).astype(BF16)
    d_probs = dot('qkgd,skd->kgqs', d_attn, v_states)
    d_scores = (attn_probs * (d_probs - jnp.sum(attn_probs * d_probs, axis=-1, keepdims=True)) / math.sqrt(HEAD_DIM)).astype(BF16)
    d_q_rot = dot('kgqs,skd->qkgd', d_scores, k_states).astype(BF16).astype(F32).reshape(n_seq, n_heads, HEAD_DIM)
    d_k_rot = dot('kgqs,qkgd->skd', d_scores, q_states).astype(BF16).astype(F32)
    d_q_lin = (d_q_rot * cos_t + rotate_half_t(d_q_rot * sin_t)).reshape(n_seq, q_width)
    d_k_lin = (d_k_rot * cos_t + rotate_half_t(d_k_rot * sin_t)).reshape(n_seq, kv_width)
    d_v_lin = d_v_states.reshape(n_seq, kv_width)
    d_b_q = jnp.sum(d_q_lin, axis=0)
    d_b_k = jnp.sum(d_k_lin, axis=0)
    d_b_v = jnp.sum(d_v_lin.astype(F32), axis=0)
    d_qkv = jnp.concatenate([d_q_lin.astype(BF16), d_k_lin.astype(BF16), d_v_lin], axis=1)
    d_w_qkv = dot('sd,se->de', normed_attn, d_qkv)
    d_normed_attn = dot('se,de->sd', d_qkv, w_qkv).astype(BF16).astype(F32)
    d_hidden_norm, d_gain_a = norm_bwd(hidden, inv_attn, gain_a, d_normed_attn)
    grad_hidden = (d_resid.astype(F32) + d_hidden_norm).astype(BF16)

    g_w_o = lax.psum_scatter(d_w_o, AX, scatter_dimension=0, tiled=True)
    d_kvb = jnp.concatenate([d_b_k.reshape(N_DEV, n_b), d_b_v.reshape(N_DEV, n_b), jnp.zeros((N_DEV, rows - 2 * n_b), F32)], axis=1)
    d_small = jnp.stack([d_gain_a, d_b_q, d_gain_m, d_kvb.reshape(width)], axis=1)
    d_small = jnp.pad(d_small, ((0, 0), (0, 124)))
    g_qkv = lax.psum_scatter(jnp.concatenate([d_w_qkv, d_small], axis=1), AX, scatter_dimension=0, tiled=True)
    g_w_q = g_qkv[:, :q_width]
    g_w_k = g_qkv[:, q_width:q_width + kv_width]
    g_w_v = g_qkv[:, q_width + kv_width:n_qkv]
    g_small = g_qkv[:, n_qkv:n_qkv + 4].T
    g_kvb = g_small[3]
    return (layer_out[None], grad_hidden[None], g_small[0], g_w_q, g_small[1], g_w_k, g_kvb[:n_b], g_w_v, g_kvb[n_b:2 * n_b],
            g_w_o, g_small[2], g_w_gate, g_w_up, g_w_down)


def solution(mesh):
    act_spec = P(AX, None, None)
    mat_spec = P(AX, None)
    vec_spec = P(AX)
    param_specs = (vec_spec, mat_spec, vec_spec, mat_spec, vec_spec, mat_spec, vec_spec, mat_spec, vec_spec, mat_spec, mat_spec, mat_spec)
    in_specs_all = (act_spec, act_spec, mat_spec) + param_specs
    out_specs_all = (act_spec, act_spec) + param_specs
    return jax.shard_map(local_step, mesh=mesh, in_specs=in_specs_all, out_specs=out_specs_all, check_vma=False)
```

```python
import math
import jax
import jax.numpy as jnp
from jax import lax
from jax.experimental import pallas as pl
from jax.experimental.pallas import tpu as pltpu
from jax.sharding import PartitionSpec as P

HEAD_DIM = 128
NORM_EPS = 1e-6
ROPE_THETA = 1000000.0
AX = 'fsdp'
N_DEV = 16
TP = 8
GROUPS = [list(range(0, 8)), list(range(8, 16))]
Z_PERM = [(i, i ^ 8) for i in range(N_DEV)]
F32 = jnp.float32
BF16 = jnp.bfloat16
CHUNKS = 2


def dot(eq_form, lhs_arr, rhs_arr):
    return jnp.einsum(eq_form, lhs_arr, rhs_arr, preferred_element_type=F32)


def rope_tables(positions):
    inv_freq = 1.0 / jnp.power(ROPE_THETA, jnp.arange(0, HEAD_DIM, 2).astype(F32) / HEAD_DIM)
    angles = positions.astype(F32)[:, None] * inv_freq
    cos_h, sin_h = jnp.cos(angles), jnp.sin(angles)
    return jnp.concatenate([cos_h, cos_h], axis=-1), jnp.concatenate([-sin_h, sin_h], axis=-1)


def rope(vec, cos_t, sin_t):
    return vec * cos_t + pltpu.roll(vec, HEAD_DIM // 2, 1) * sin_t


def rope_t(vec, cos_t, sin_t):
    return vec * cos_t - pltpu.roll(vec, HEAD_DIM // 2, 1) * sin_t


def dot_nt(lhs, rhs):
    return lax.dot_general(lhs, rhs, (((1,), (1,)), ((), ())), preferred_element_type=F32)


def dot_nn(lhs, rhs):
    return lax.dot_general(lhs, rhs, (((1,), (0,)), ((), ())), preferred_element_type=F32)


def dot_tn(lhs, rhs):
    return lax.dot_general(lhs, rhs, (((0,), (0,)), ((), ())), preferred_element_type=F32)


SCALE = 1.0 / math.sqrt(HEAD_DIM)


def attn_fwd_kernel(q_ref, k_ref, v_ref, cos_ref, sin_ref, o_ref):
    cos_t, sin_t = cos_ref[...], sin_ref[...]
    q_rot = rope(q_ref[...], cos_t, sin_t).astype(BF16)
    k_rot = rope(k_ref[...], cos_t, sin_t).astype(BF16)
    scores = dot_nt(q_rot, k_rot) * SCALE
    keep = lax.broadcasted_iota(jnp.int32, scores.shape, 0) >= lax.broadcasted_iota(jnp.int32, scores.shape, 1)
    scores = jnp.where(keep, scores, -1e30)
    probs = jnp.exp(scores - jnp.max(scores, axis=1, keepdims=True))
    probs = probs * (1.0 / jnp.sum(probs, axis=1, keepdims=True))
    o_ref[...] = dot_nn(probs.astype(BF16), v_ref[...].astype(BF16)).astype(BF16)


def attn_fwd(qkv, cos_t, sin_t, n_heads, n_kv):
    n_seq = qkv.shape[0]
    group = n_heads // n_kv
    tab = pl.BlockSpec((n_seq, HEAD_DIM), lambda h: (0, 0))
    return pl.pallas_call(
        attn_fwd_kernel,
        grid=(n_heads,),
        in_specs=[
            pl.BlockSpec((n_seq, HEAD_DIM), lambda h: (0, h)),
            pl.BlockSpec((n_seq, HEAD_DIM), lambda h: (0, n_heads + h // group)),
            pl.BlockSpec((n_seq, HEAD_DIM), lambda h: (0, n_heads + n_kv + h // group)),
            tab, tab,
        ],
        out_specs=pl.BlockSpec((n_seq, HEAD_DIM), lambda h: (0, h)),
        out_shape=jax.ShapeDtypeStruct((n_seq, n_heads * HEAD_DIM), BF16),
        compiler_params=pltpu.CompilerParams(vmem_limit_bytes=40 << 20),
        cost_estimate=pl.CostEstimate(flops=8 << 30, bytes_accessed=6 << 20, transcendentals=3 << 20),
        name='attn_fwd',
    )(qkv, qkv, qkv, cos_t, sin_t)


def attn_bwd_kernel(q_ref, k_ref, v_ref, do_ref, cos_ref, sin_ref, dq_ref, dk_ref, dv_ref, bq_ref, bk_ref, bv_ref, dk_acc, dv_acc):
    step = pl.program_id(1)
    cos_t, sin_t = cos_ref[...], sin_ref[...]
    q_rot = rope(q_ref[...], cos_t, sin_t).astype(BF16)
    k_rot = rope(k_ref[...], cos_t, sin_t).astype(BF16)
    v_st = v_ref[...].astype(BF16)
    d_out = do_ref[...]
    scores = dot_nt(k_rot, q_rot) * SCALE
    keep = lax.broadcasted_iota(jnp.int32, scores.shape, 1) >= lax.broadcasted_iota(jnp.int32, scores.shape, 0)
    scores = jnp.where(keep, scores, -1e30)
    probs = jnp.exp(scores - jnp.max(scores, axis=0, keepdims=True))
    probs = probs * (1.0 / jnp.sum(probs, axis=0, keepdims=True))
    d_v = dot_nn(probs.astype(BF16), d_out)
    d_probs = dot_nt(v_st, d_out)
    d_sc = (probs * (d_probs - jnp.sum(probs * d_probs, axis=0, keepdims=True)) * SCALE).astype(BF16)
    d_k = dot_nn(d_sc, q_rot)
    d_q = dot_tn(d_sc, k_rot).astype(BF16).astype(F32)
    d_q = rope_t(d_q, cos_t, sin_t)
    dq_ref[...] = d_q.astype(BF16)
    bq_ref[...] = jnp.sum(d_q, axis=0, keepdims=True)

    @pl.when(step == 0)
    def _():
        dk_acc[...] = d_k
        dv_acc[...] = d_v

    @pl.when(step > 0)
    def _():
        dk_acc[...] += d_k
        dv_acc[...] += d_v

    @pl.when(step == pl.num_programs(1) - 1)
    def _():
        d_k_all = rope_t(dk_acc[...].astype(BF16).astype(F32), cos_t, sin_t)
        dk_ref[...] = d_k_all.astype(BF16)
        bk_ref[...] = jnp.sum(d_k_all, axis=0, keepdims=True)
        d_v_all = dv_acc[...].astype(BF16)
        dv_ref[...] = d_v_all
        bv_ref[...] = jnp.sum(d_v_all.astype(F32), axis=0, keepdims=True)


def attn_bwd(qkv, d_attn, cos_t, sin_t, n_heads, n_kv):
    n_seq = qkv.shape[0]
    group = n_heads // n_kv
    tab = pl.BlockSpec((n_seq, HEAD_DIM), lambda j, g: (0, 0))
    blk_h = pl.BlockSpec((n_seq, HEAD_DIM), lambda j, g: (0, j * group + g))
    blk_kv = pl.BlockSpec((n_seq, HEAD_DIM), lambda j, g: (0, j))
    vec_h = pl.BlockSpec((1, HEAD_DIM), lambda j, g: (0, j * group + g))
    vec_kv = pl.BlockSpec((1, HEAD_DIM), lambda j, g: (0, j))
    q_width, kv_width = n_heads * HEAD_DIM, n_kv * HEAD_DIM
    return pl.pallas_call(
        attn_bwd_kernel,
        grid=(n_kv, group),
        in_specs=[
            blk_h,
            pl.BlockSpec((n_seq, HEAD_DIM), lambda j, g: (0, n_heads + j)),
            pl.BlockSpec((n_seq, HEAD_DIM), lambda j, g: (0, n_heads + n_kv + j)),
            blk_h, tab, tab,
        ],
        out_specs=[blk_h, blk_kv, blk_kv, vec_h, vec_kv, vec_kv],
        out_shape=[
            jax.ShapeDtypeStruct((n_seq, q_width), BF16),
            jax.ShapeDtypeStruct((n_seq, kv_width), BF16),
            jax.ShapeDtypeStruct((n_seq, kv_width), BF16),
            jax.ShapeDtypeStruct((1, q_width), F32),
            jax.ShapeDtypeStruct((1, kv_width), F32),
            jax.ShapeDtypeStruct((1, kv_width), F32),
        ],
        scratch_shapes=[pltpu.VMEM((n_seq, HEAD_DIM), F32), pltpu.VMEM((n_seq, HEAD_DIM), F32)],
        compiler_params=pltpu.CompilerParams(vmem_limit_bytes=40 << 20),
        cost_estimate=pl.CostEstimate(flops=16 << 30, bytes_accessed=10 << 20, transcendentals=3 << 20),
        name='attn_bwd',
    )(qkv, qkv, qkv, d_attn, cos_t, sin_t)


GRAD_BLK = 256


def attn_grads_kernel(n_o, n_all, lhs_o_ref, lhs_h_ref, rhs_o_ref, rhs_h_ref, small_ref, out_ref):
    step = pl.program_id(0)

    @pl.when(step < n_o)
    def _():
        out_ref[...] = dot_nn(lhs_o_ref[...], rhs_o_ref[...])

    @pl.when(jnp.logical_and(step >= n_o, step < n_all))
    def _():
        out_ref[...] = dot_nn(lhs_h_ref[...], rhs_h_ref[...])

    @pl.when(step == n_all)
    def _():
        out_ref[...] = small_ref[...]


def attn_grads(lhs_o, rhs_o, lhs_h, rhs_h, small):
    width, n_seq = lhs_o.shape
    n_o, n_h = rhs_o.shape[1] // GRAD_BLK, rhs_h.shape[1] // GRAD_BLK
    n_all = n_o + n_h
    full = pl.BlockSpec((width, n_seq), lambda j: (0, 0))
    return pl.pallas_call(
        lambda *refs: attn_grads_kernel(n_o, n_all, *refs),
        grid=(n_all + 1,),
        in_specs=[
            full, full,
            pl.BlockSpec((n_seq, GRAD_BLK), lambda j: (0, jnp.minimum(j, n_o - 1))),
            pl.BlockSpec((n_seq, GRAD_BLK), lambda j: (0, jnp.clip(j - n_o, 0, n_h - 1))),
            pl.BlockSpec((width, GRAD_BLK), lambda j: (0, 0)),
        ],
        out_specs=pl.BlockSpec((width, GRAD_BLK), lambda j: (0, j)),
        out_shape=jax.ShapeDtypeStruct((width, (n_all + 1) * GRAD_BLK), F32),
        compiler_params=pltpu.CompilerParams(vmem_limit_bytes=40 << 20),
        cost_estimate=pl.CostEstimate(flops=12 << 30, bytes_accessed=32 << 20, transcendentals=0),
        name='attn_grads',
    )(lhs_o, lhs_h, rhs_o, rhs_h, small)


def norm_fwd(hidden, gain_vec):
    x_f32 = hidden.astype(F32)
    inv_rms = lax.rsqrt(jnp.mean(x_f32 * x_f32, axis=-1, keepdims=True) + NORM_EPS)
    return (x_f32 * inv_rms * gain_vec).astype(BF16), inv_rms


def norm_bwd(hidden, inv_rms, gain_vec, d_normed):
    unit_rows = hidden.astype(F32) * inv_rms
    d_gain = jnp.sum(d_normed * unit_rows, axis=0)
    d_unit = d_normed * gain_vec
    d_hidden = inv_rms * (d_unit - unit_rows * jnp.mean(d_unit * unit_rows, axis=-1, keepdims=True))
    return d_hidden, d_gain


def z_pair(arr):
    return lax.ppermute(arr, AX, Z_PERM)


barrier = lax.optimization_barrier


def group_gather(arr):
    return lax.all_gather(arr, AX, axis=0, tiled=True, axis_index_groups=GROUPS)


def group_scatter(arr):
    return lax.psum_scatter(arr, AX, scatter_dimension=0, tiled=True, axis_index_groups=GROUPS)


def local_step(hidden, grad_out, positions, gain_attn, w_q, b_q, w_k, b_k, w_v, b_v, w_o, gain_mlp, w_gate, w_up, w_down):
    n_seq, width = hidden.shape[1], hidden.shape[2]
    rows = w_q.shape[0]
    q_width, kv_width = w_q.shape[1], w_k.shape[1]
    n_heads, n_kv = q_width // HEAD_DIM, kv_width // HEAD_DIM
    ff_blk = w_down.shape[0]
    ff_loc = 2 * ff_blk
    half = width // 2
    dev = lax.axis_index(AX)
    z_idx, rank = dev // TP, dev % TP
    z_zero = z_idx == 0
    hidden = hidden[0]
    grad_out = grad_out[0]

    kvb = jnp.concatenate([b_k, b_v, jnp.zeros((rows - 2 * b_k.shape[0],), BF16)])
    small = jnp.stack([gain_attn, b_q, gain_mlp, kvb], axis=1)
    small = jnp.pad(small, ((0, 0), (0, 124)))
    qkv_loc = jnp.concatenate([w_q, w_k, w_v, small], axis=1)
    qkv_full = lax.all_gather(qkv_loc, AX, axis=0, tiled=True)
    n_qkv = q_width + 2 * kv_width
    w_o_full = lax.all_gather(w_o, AX, axis=0, tiled=True)
    down_other = z_pair(w_down)

    gu = jnp.stack([w_gate, w_up], axis=0).reshape(2, rows, 2, TP, ff_blk)
    gu = gu.transpose(3, 0, 1, 2, 4).reshape(TP, 2, rows, ff_loc)
    gu, hidden = barrier((gu, hidden))
    gu_rows = jnp.zeros((2, TP, rows, ff_loc), BF16)
    for d in range(TP):
        piece = lax.dynamic_index_in_dim(gu, rank ^ d, 0, keepdims=False)
        if d:
            piece = lax.ppermute(piece, AX, [(i, i ^ d) for i in range(N_DEV)])
        gu_rows = lax.dynamic_update_slice(gu_rows, piece[:, None], (0, rank ^ d, 0, 0))
    gu_rows = gu_rows.reshape(2, half, ff_loc)

    w_qkv = qkv_full[:, :n_qkv]
    small_t = qkv_full[:, n_qkv:n_qkv + 4].T.astype(F32)
    gain_a, bias_q, gain_m = small_t[0], small_t[1], small_t[2]
    kvb_full = small_t[3].reshape(N_DEV, rows)
    n_b = b_k.shape[0]
    bias = jnp.concatenate([bias_q, kvb_full[:, :n_b].reshape(kv_width), kvb_full[:, n_b:2 * n_b].reshape(kv_width)])
    cos_t, sin_t = rope_tables(positions[0])
    normed_attn, inv_attn = norm_fwd(hidden, gain_a)
    qkv = dot('sd,de->se', normed_attn, w_qkv) + bias
    qkv, gu_rows = barrier((qkv, gu_rows))
    gu_other = z_pair(gu_rows)
    attn_out = attn_fwd(qkv, cos_t, sin_t, n_heads, n_kv)
    resid_mid = (hidden.astype(F32) + dot('se,ed->sd', attn_out, w_o_full)).astype(BF16)
    normed_mlp, inv_mlp = norm_fwd(resid_mid, gain_m)
    normed_mlp, grad_out = barrier((normed_mlp, grad_out))

    n_ch = n_seq // CHUNKS
    h_all = [group_gather(normed_mlp[c * n_ch:(c + 1) * n_ch]) for c in range(CHUNKS)]
    go_all = [group_gather(grad_out[c * n_ch:(c + 1) * n_ch]) for c in range(CHUNKS)]

    gu_lo = jnp.where(z_zero, gu_rows, gu_other)
    gu_hi = jnp.where(z_zero, gu_other, gu_rows)
    w_g = jnp.concatenate([gu_lo[0], gu_hi[0]], axis=0)
    w_u = jnp.concatenate([gu_lo[1], gu_hi[1]], axis=0)
    w_d = jnp.concatenate([jnp.where(z_zero, w_down, down_other), jnp.where(z_zero, down_other, w_down)], axis=0)

    pre = []
    for c in range(CHUNKS):
        gate_pre = dot('sd,df->sf', h_all[c], w_g)
        up_proj = dot('sd,df->sf', h_all[c], w_u)
        pre.append((gate_pre, up_proj))
    acts, d_gates, d_ups, dn_sums = [], [], [], []
    for c in range(CHUNKS):
        gate_pre, up_proj = pre[c]
        act = (jax.nn.silu(gate_pre) * up_proj).astype(BF16)
        d_act = dot('sd,fd->sf', go_all[c], w_d).astype(BF16).astype(F32)
        gate_sig = jax.nn.sigmoid(gate_pre)
        d_gate = (d_act * up_proj * gate_sig * (1.0 + gate_pre * (1.0 - gate_sig))).astype(BF16)
        d_up = (d_act * gate_pre * gate_sig).astype(BF16)
        dn_part = dot('sf,df->sd', d_gate, w_g) + dot('sf,df->sd', d_up, w_u)
        dn_sums.append(group_scatter(dn_part))
        acts.append(act)
        d_gates.append(d_gate)
        d_ups.append(d_up)
    dn_part, acts, d_gates, d_ups, h_all = barrier((dn_part, acts, d_gates, d_ups, h_all))

    def token_dot(eq_form, lhs_list, rhs_list):
        total = dot(eq_form, lhs_list[0], rhs_list[0])
        for lhs, rhs in zip(lhs_list[1:], rhs_list[1:]):
            total = total + dot(eq_form, lhs, rhs)
        return total

    h_send = [lax.dynamic_slice_in_dim(h, (1 - z_idx) * half, half, axis=1) for h in h_all]
    h_keep = [lax.dynamic_slice_in_dim(h, z_idx * half, half, axis=1) for h in h_all]
    gg_send = token_dot('sd,sf->df', h_send, d_gates)
    gu_send = token_dot('sd,sf->df', h_send, d_ups)
    d_wd = token_dot('sf,sd->fd', acts, go_all)
    wd_send = lax.dynamic_slice_in_dim(d_wd, (1 - z_idx) * ff_blk, ff_blk, axis=0)
    wd_keep = lax.dynamic_slice_in_dim(d_wd, z_idx * ff_blk, ff_blk, axis=0)
    gg_recv, gu_recv, wd_recv = z_pair(gg_send), z_pair(gu_send), z_pair(wd_send)
    gg_keep = token_dot('sd,sf->df', h_keep, d_gates)
    gu_keep = token_dot('sd,sf->df', h_keep, d_ups)
    out_part = [dot('sf,fd->sd', act, w_d) for act in acts]
    dn_sums, gg_keep, gu_keep, out_part, wd_keep = barrier((dn_sums, gg_keep, gu_keep, out_part, wd_keep))
    d_normed_mlp = jnp.concatenate(dn_sums, axis=0).astype(BF16).astype(F32)
    out_sum = jnp.concatenate([group_scatter(part) for part in out_part], axis=0)
    g_w_down = wd_keep + wd_recv

    def back_rows(grad):
        grad = lax.all_to_all(grad.reshape(TP, rows, ff_loc), AX, 0, 0, axis_index_groups=GROUPS, tiled=True)
        return grad.reshape(TP, rows, 2, ff_blk).transpose(1, 2, 0, 3).reshape(rows, N_DEV * ff_blk)

    g_w_gate = back_rows(gg_keep + gg_recv)
    g_w_up = back_rows(gu_keep + gu_recv)

    d_resid_norm, d_gain_m = norm_bwd(resid_mid, inv_mlp, gain_m, d_normed_mlp)
    d_resid = (grad_out.astype(F32) + d_resid_norm).astype(BF16)
    d_attn = dot('sd,ed->se', d_resid, w_o_full).astype(BF16)
    d_q, d_k, d_v, d_b_q, d_b_k, d_b_v = attn_bwd(qkv, d_attn, cos_t, sin_t, n_heads, n_kv)
    d_qkv = jnp.concatenate([d_q, d_k, d_v], axis=1)
    d_normed_attn = dot('se,de->sd', d_qkv, w_qkv).astype(BF16).astype(F32)
    d_hidden_norm, d_gain_a = norm_bwd(hidden, inv_attn, gain_a, d_normed_attn)
    grad_hidden = (d_resid.astype(F32) + d_hidden_norm).astype(BF16)

    d_kvb = jnp.concatenate([d_b_k.reshape(N_DEV, n_b), d_b_v.reshape(N_DEV, n_b), jnp.zeros((N_DEV, rows - 2 * n_b), F32)], axis=1)
    d_small = jnp.stack([d_gain_a, d_b_q[0], d_gain_m, d_kvb.reshape(width)], axis=1)
    d_small = jnp.pad(d_small, ((0, 0), (0, GRAD_BLK - 4)))
    grads = attn_grads(attn_out.T, d_resid, normed_attn.T, d_qkv, d_small)
    grads = lax.psum_scatter(grads, AX, scatter_dimension=0, tiled=True)
    out_sum, grads = barrier((out_sum, grads))
    layer_out = (resid_mid.astype(F32) + out_sum).astype(BF16)
    g_w_o, g_qkv = grads[:, :width], grads[:, width:]
    g_w_q = g_qkv[:, :q_width]
    g_w_k = g_qkv[:, q_width:q_width + kv_width]
    g_w_v = g_qkv[:, q_width + kv_width:n_qkv]
    g_small = g_qkv[:, n_qkv:n_qkv + 4].T
    g_kvb = g_small[3]
    return (layer_out[None], grad_hidden[None], g_small[0], g_w_q, g_small[1], g_w_k, g_kvb[:n_b], g_w_v, g_kvb[n_b:2 * n_b],
            g_w_o, g_small[2], g_w_gate, g_w_up, g_w_down)


def solution(mesh):
    act_spec = P(AX, None, None)
    mat_spec = P(AX, None)
    vec_spec = P(AX)
    param_specs = (vec_spec, mat_spec, vec_spec, mat_spec, vec_spec, mat_spec, vec_spec, mat_spec, vec_spec, mat_spec, mat_spec, mat_spec)
    in_specs_all = (act_spec, act_spec, mat_spec) + param_specs
    out_specs_all = (act_spec, act_spec) + param_specs

    return jax.shard_map(local_step, mesh=mesh, in_specs=in_specs_all, out_specs=out_specs_all, check_vma=False)
```

```python
import math
import jax
import jax.numpy as jnp
from jax import lax
from jax.experimental import pallas as pl
from jax.experimental.pallas import tpu as pltpu
from jax.sharding import PartitionSpec as P

HEAD_DIM = 128
NORM_EPS = 1e-6
ROPE_THETA = 1000000.0
AX = 'fsdp'
N_DEV = 16
TP = 8
GROUPS = [list(range(0, 8)), list(range(8, 16))]
Z_PERM = [(i, i ^ 8) for i in range(N_DEV)]
F32 = jnp.float32
BF16 = jnp.bfloat16
CHUNKS = 2


def dot(eq_form, lhs_arr, rhs_arr):
    return jnp.einsum(eq_form, lhs_arr, rhs_arr, preferred_element_type=F32)


def rope_tables(positions):
    inv_freq = 1.0 / jnp.power(ROPE_THETA, jnp.arange(0, HEAD_DIM, 2).astype(F32) / HEAD_DIM)
    angles = positions.astype(F32)[:, None] * inv_freq
    cos_h, sin_h = jnp.cos(angles), jnp.sin(angles)
    return jnp.concatenate([cos_h, cos_h], axis=-1), jnp.concatenate([-sin_h, sin_h], axis=-1)


def rope(vec, cos_t, sin_t):
    return vec * cos_t + pltpu.roll(vec, HEAD_DIM // 2, 1) * sin_t


def rope_t(vec, cos_t, sin_t):
    return vec * cos_t - pltpu.roll(vec, HEAD_DIM // 2, 1) * sin_t


def dot_nt(lhs, rhs):
    return lax.dot_general(lhs, rhs, (((1,), (1,)), ((), ())), preferred_element_type=F32)


def dot_nn(lhs, rhs):
    return lax.dot_general(lhs, rhs, (((1,), (0,)), ((), ())), preferred_element_type=F32)


def dot_tn(lhs, rhs):
    return lax.dot_general(lhs, rhs, (((0,), (0,)), ((), ())), preferred_element_type=F32)


SCALE = 1.0 / math.sqrt(HEAD_DIM)


def attn_fwd_kernel(q_ref, k_ref, v_ref, cos_ref, sin_ref, o_ref):
    cos_t, sin_t = cos_ref[...], sin_ref[...]
    q_rot = rope(q_ref[...], cos_t, sin_t).astype(BF16)
    k_rot = rope(k_ref[...], cos_t, sin_t).astype(BF16)
    scores = dot_nt(q_rot, k_rot) * SCALE
    keep = lax.broadcasted_iota(jnp.int32, scores.shape, 0) >= lax.broadcasted_iota(jnp.int32, scores.shape, 1)
    scores = jnp.where(keep, scores, -1e30)
    probs = jnp.exp(scores - jnp.max(scores, axis=1, keepdims=True))
    probs = probs * (1.0 / jnp.sum(probs, axis=1, keepdims=True))
    o_ref[...] = dot_nn(probs.astype(BF16), v_ref[...].astype(BF16)).astype(BF16)


def attn_fwd(qkv, cos_t, sin_t, n_heads, n_kv):
    n_seq = qkv.shape[0]
    group = n_heads // n_kv
    tab = pl.BlockSpec((n_seq, HEAD_DIM), lambda h: (0, 0))
    return pl.pallas_call(
        attn_fwd_kernel,
        grid=(n_heads,),
        in_specs=[
            pl.BlockSpec((n_seq, HEAD_DIM), lambda h: (0, h)),
            pl.BlockSpec((n_seq, HEAD_DIM), lambda h: (0, n_heads + h // group)),
            pl.BlockSpec((n_seq, HEAD_DIM), lambda h: (0, n_heads + n_kv + h // group)),
            tab, tab,
        ],
        out_specs=pl.BlockSpec((n_seq, HEAD_DIM), lambda h: (0, h)),
        out_shape=jax.ShapeDtypeStruct((n_seq, n_heads * HEAD_DIM), BF16),
        compiler_params=pltpu.CompilerParams(vmem_limit_bytes=40 << 20),
        cost_estimate=pl.CostEstimate(flops=8 << 30, bytes_accessed=6 << 20, transcendentals=3 << 20),
        name='attn_fwd',
    )(qkv, qkv, qkv, cos_t, sin_t)


def attn_bwd_kernel(q_ref, k_ref, v_ref, do_ref, cos_ref, sin_ref, dq_ref, dk_ref, dv_ref, bq_ref, bk_ref, bv_ref, dk_acc, dv_acc):
    step = pl.program_id(1)
    cos_t, sin_t = cos_ref[...], sin_ref[...]
    q_rot = rope(q_ref[...], cos_t, sin_t).astype(BF16)
    k_rot = rope(k_ref[...], cos_t, sin_t).astype(BF16)
    v_st = v_ref[...].astype(BF16)
    d_out = do_ref[...]
    scores = dot_nt(k_rot, q_rot) * SCALE
    keep = lax.broadcasted_iota(jnp.int32, scores.shape, 1) >= lax.broadcasted_iota(jnp.int32, scores.shape, 0)
    scores = jnp.where(keep, scores, -1e30)
    probs = jnp.exp(scores - jnp.max(scores, axis=0, keepdims=True))
    probs = probs * (1.0 / jnp.sum(probs, axis=0, keepdims=True))
    d_v = dot_nn(probs.astype(BF16), d_out)
    d_probs = dot_nt(v_st, d_out)
    d_sc = (probs * (d_probs - jnp.sum(probs * d_probs, axis=0, keepdims=True)) * SCALE).astype(BF16)
    d_k = dot_nn(d_sc, q_rot)
    d_q = dot_tn(d_sc, k_rot).astype(BF16).astype(F32)
    d_q = rope_t(d_q, cos_t, sin_t)
    dq_ref[...] = d_q.astype(BF16)
    bq_ref[...] = jnp.sum(d_q, axis=0, keepdims=True)

    @pl.when(step == 0)
    def _():
        dk_acc[...] = d_k
        dv_acc[...] = d_v

    @pl.when(step > 0)
    def _():
        dk_acc[...] += d_k
        dv_acc[...] += d_v

    @pl.when(step == pl.num_programs(1) - 1)
    def _():
        d_k_all = rope_t(dk_acc[...].astype(BF16).astype(F32), cos_t, sin_t)
        dk_ref[...] = d_k_all.astype(BF16)
        bk_ref[...] = jnp.sum(d_k_all, axis=0, keepdims=True)
        d_v_all = dv_acc[...].astype(BF16)
        dv_ref[...] = d_v_all
        bv_ref[...] = jnp.sum(d_v_all.astype(F32), axis=0, keepdims=True)


def attn_bwd(qkv, d_attn, cos_t, sin_t, n_heads, n_kv):
    n_seq = qkv.shape[0]
    group = n_heads // n_kv
    tab = pl.BlockSpec((n_seq, HEAD_DIM), lambda j, g: (0, 0))
    blk_h = pl.BlockSpec((n_seq, HEAD_DIM), lambda j, g: (0, j * group + g))
    blk_kv = pl.BlockSpec((n_seq, HEAD_DIM), lambda j, g: (0, j))
    vec_h = pl.BlockSpec((1, HEAD_DIM), lambda j, g: (0, j * group + g))
    vec_kv = pl.BlockSpec((1, HEAD_DIM), lambda j, g: (0, j))
    q_width, kv_width = n_heads * HEAD_DIM, n_kv * HEAD_DIM
    return pl.pallas_call(
        attn_bwd_kernel,
        grid=(n_kv, group),
        in_specs=[
            blk_h,
            pl.BlockSpec((n_seq, HEAD_DIM), lambda j, g: (0, n_heads + j)),
            pl.BlockSpec((n_seq, HEAD_DIM), lambda j, g: (0, n_heads + n_kv + j)),
            blk_h, tab, tab,
        ],
        out_specs=[blk_h, blk_kv, blk_kv, vec_h, vec_kv, vec_kv],
        out_shape=[
            jax.ShapeDtypeStruct((n_seq, q_width), BF16),
            jax.ShapeDtypeStruct((n_seq, kv_width), BF16),
            jax.ShapeDtypeStruct((n_seq, kv_width), BF16),
            jax.ShapeDtypeStruct((1, q_width), F32),
            jax.ShapeDtypeStruct((1, kv_width), F32),
            jax.ShapeDtypeStruct((1, kv_width), F32),
        ],
        scratch_shapes=[pltpu.VMEM((n_seq, HEAD_DIM), F32), pltpu.VMEM((n_seq, HEAD_DIM), F32)],
        compiler_params=pltpu.CompilerParams(vmem_limit_bytes=40 << 20),
        cost_estimate=pl.CostEstimate(flops=16 << 30, bytes_accessed=10 << 20, transcendentals=3 << 20),
        name='attn_bwd',
    )(qkv, qkv, qkv, d_attn, cos_t, sin_t)


GRAD_BLK = 256


def attn_grads_kernel(n_o, n_all, lhs_o_ref, lhs_h_ref, rhs_o_ref, rhs_h_ref, small_ref, out_ref):
    step = pl.program_id(0)

    @pl.when(step < n_o)
    def _():
        out_ref[...] = dot_nn(lhs_o_ref[...], rhs_o_ref[...])

    @pl.when(jnp.logical_and(step >= n_o, step < n_all))
    def _():
        out_ref[...] = dot_nn(lhs_h_ref[...], rhs_h_ref[...])

    @pl.when(step == n_all)
    def _():
        out_ref[...] = small_ref[...]


def attn_grads(lhs_o, rhs_o, lhs_h, rhs_h, small):
    width, n_seq = lhs_o.shape
    n_o, n_h = rhs_o.shape[1] // GRAD_BLK, rhs_h.shape[1] // GRAD_BLK
    n_all = n_o + n_h
    full = pl.BlockSpec((width, n_seq), lambda j: (0, 0))
    return pl.pallas_call(
        lambda *refs: attn_grads_kernel(n_o, n_all, *refs),
        grid=(n_all + 1,),
        in_specs=[
            full, full,
            pl.BlockSpec((n_seq, GRAD_BLK), lambda j: (0, jnp.minimum(j, n_o - 1))),
            pl.BlockSpec((n_seq, GRAD_BLK), lambda j: (0, jnp.clip(j - n_o, 0, n_h - 1))),
            pl.BlockSpec((width, GRAD_BLK), lambda j: (0, 0)),
        ],
        out_specs=pl.BlockSpec((width, GRAD_BLK), lambda j: (0, j)),
        out_shape=jax.ShapeDtypeStruct((width, (n_all + 1) * GRAD_BLK), F32),
        compiler_params=pltpu.CompilerParams(vmem_limit_bytes=40 << 20),
        cost_estimate=pl.CostEstimate(flops=12 << 30, bytes_accessed=32 << 20, transcendentals=0),
        name='attn_grads',
    )(lhs_o, lhs_h, rhs_o, rhs_h, small)


def norm_fwd(hidden, gain_vec):
    x_f32 = hidden.astype(F32)
    inv_rms = lax.rsqrt(jnp.mean(x_f32 * x_f32, axis=-1, keepdims=True) + NORM_EPS)
    return (x_f32 * inv_rms * gain_vec).astype(BF16), inv_rms


def norm_bwd(hidden, inv_rms, gain_vec, d_normed):
    unit_rows = hidden.astype(F32) * inv_rms
    d_gain = jnp.sum(d_normed * unit_rows, axis=0)
    d_unit = d_normed * gain_vec
    d_hidden = inv_rms * (d_unit - unit_rows * jnp.mean(d_unit * unit_rows, axis=-1, keepdims=True))
    return d_hidden, d_gain


def cut_kernel(blk, n_rank, gate_ref, up_ref, out_ref):
    for r in range(n_rank):
        for g, src in enumerate((gate_ref, up_ref)):
            out_ref[r, g, :, 0:blk] = src[:, r * blk:(r + 1) * blk]
            out_ref[r, g, :, blk:2 * blk] = src[:, (n_rank + r) * blk:(n_rank + r + 1) * blk]


def cut_columns(w_gate, w_up, blk):
    rows = w_gate.shape[0]
    return pl.pallas_call(
        lambda *refs: cut_kernel(blk, TP, *refs),
        out_shape=jax.ShapeDtypeStruct((TP, 2, rows, 2 * blk), BF16),
        in_specs=[pl.BlockSpec(memory_space=pltpu.VMEM)] * 2,
        out_specs=pl.BlockSpec(memory_space=pltpu.VMEM),
        compiler_params=pltpu.CompilerParams(vmem_limit_bytes=24 << 20),
        cost_estimate=pl.CostEstimate(flops=4 << 30, bytes_accessed=8 << 20, transcendentals=0),
        name='cut_columns',
    )(w_gate, w_up)


def join_kernel(blk, n_rank, src_ref, out_ref):
    for r in range(n_rank):
        out_ref[:, r * blk:(r + 1) * blk] = src_ref[r, :, 0:blk]
        out_ref[:, (n_rank + r) * blk:(n_rank + r + 1) * blk] = src_ref[r, :, blk:2 * blk]


def join_columns(parts, blk):
    rows = parts.shape[1]
    tile = 32
    return pl.pallas_call(
        lambda *refs: join_kernel(blk, TP, *refs),
        grid=(rows // tile,),
        out_shape=jax.ShapeDtypeStruct((rows, 2 * TP * blk), F32),
        in_specs=[pl.BlockSpec((TP, tile, 2 * blk), lambda i: (0, i, 0))],
        out_specs=pl.BlockSpec((tile, 2 * TP * blk), lambda i: (i, 0)),
        compiler_params=pltpu.CompilerParams(vmem_limit_bytes=24 << 20),
        cost_estimate=pl.CostEstimate(flops=4 << 30, bytes_accessed=8 << 20, transcendentals=0),
        name='join_columns',
    )(parts)


def scatter_kernel(cols, g_ref, out_ref, own, from_core, buf1, buf2, buf3, load_sem, send_sem, recv_sem):
    dev = lax.axis_index(AX)
    me = (dev // 8, (dev // 4) % 2, (dev // 2) % 2)
    core = dev % 2
    peer_core = dev + 1 - 2 * core
    peers = tuple(dev + step * (1 - 2 * pos) for step, pos in zip((8, 4, 2), me))
    barrier_sem = pltpu.get_barrier_semaphore()
    for peer in (peer_core,) + peers:
        pl.semaphore_signal(barrier_sem, inc=1, device_id=(peer,), device_id_type=pl.DeviceIdType.MESH)
    pl.semaphore_wait(barrier_sem, 4)
    orders = ((2, 1, 0), (1, 0, 2), (0, 2, 1))
    load = pltpu.make_async_copy(g_ref.at[:, :, :, core], own, load_sem)
    load.start()

    def pick(fixed):
        return tuple(fixed.get(d, slice(None)) for d in range(3))

    def remote(slot, src, dst, peer):
        copy = pltpu.make_async_remote_copy(
            src_ref=src, dst_ref=dst, send_sem=send_sem.at[slot], recv_sem=recv_sem.at[slot],
            device_id=(peer,), device_id_type=pl.DeviceIdType.MESH)
        copy.start()
        return copy

    def col(k):
        return pl.ds(k * cols, cols)

    core_copies = {}
    for half in range(2):
        for k, order in enumerate(orders):
            where = pick({order[0]: me[order[0]] if half else 1 - me[order[0]]})
            core_copies[half, k] = remote(
                half * 3 + k, g_ref.at[where + (1 - core, slice(None), col(k))],
                from_core.at[where + (slice(None), col(k))], peer_core)
    load.wait()

    def add(dst, src, count):
        def body(i, carry):
            a, b = i // 2, i % 2
            dst(a, b)[...] = dst(a, b)[...] + src(a, b)[...]
            return carry

        lax.fori_loop(0, count, body, 0)

    def at4(ref, k, order, first):
        def get(a, b):
            fixed = {order[0]: first, order[1]: a, order[2]: b}
            return ref.at[tuple(fixed[d] for d in range(3)) + (slice(None), col(k))]

        return get

    def at2(ref, k, order, second):
        def get(a, b):
            fixed = {order[0]: me[order[0]], order[1]: second, order[2]: b}
            return ref.at[tuple(fixed[d] for d in range(3)) + (slice(None), col(k))]

        return get

    stage1, stage2, stage3 = {}, {}, {}
    for k, order in enumerate(orders):
        core_copies[0, k].wait_recv()
        far = 1 - me[order[0]]
        add(at4(own, k, order, far), at4(from_core, k, order, far), 4)
    for k, order in enumerate(orders):
        for a in range(2):
            for b in range(2):
                fixed = {order[0]: 1 - me[order[0]], order[1]: a, order[2]: b}
                src = own.at[tuple(fixed[d] for d in range(3)) + (slice(None), col(k))]
                stage1[k, a, b] = remote(6 + k * 4 + a * 2 + b, src, buf1.at[k, a, b], peers[order[0]])
    for k, order in enumerate(orders):
        core_copies[1, k].wait_recv()
        near = me[order[0]]
        add(at4(own, k, order, near), at4(from_core, k, order, near), 4)
    for k, order in enumerate(orders):
        for a in range(2):
            for b in range(2):
                stage1[k, a, b].wait_recv()
        add(at4(own, k, order, me[order[0]]), lambda a, b, k=k: buf1.at[k, a, b], 4)
    for k, order in enumerate(orders):
        for b in range(2):
            src = at2(own, k, order, 1 - me[order[1]])(0, b)
            stage2[k, b] = remote(18 + k * 2 + b, src, buf2.at[k, b], peers[order[1]])
    for k, order in enumerate(orders):
        for b in range(2):
            stage2[k, b].wait_recv()
        add(at2(own, k, order, me[order[1]]), lambda a, b, k=k: buf2.at[k, b], 2)
    for k, order in enumerate(orders):
        src = at2(own, k, order, me[order[1]])(0, 1 - me[order[2]])
        stage3[k] = remote(24 + k, src, buf3.at[k], peers[order[2]])
    for k, order in enumerate(orders):
        stage3[k].wait_recv()
        out_ref[:, k * cols:(k + 1) * cols] = at2(own, k, order, me[order[1]])(0, me[order[2]])[...] + buf3[k]
    for copy in list(core_copies.values()) + list(stage1.values()) + list(stage2.values()) + list(stage3.values()):
        copy.wait_send()


def scatter_all(grads, rows):
    cols = grads.shape[1] // 3
    g6 = grads.reshape(2, 2, 2, 2, rows, 3 * cols)
    return pl.pallas_call(
        lambda *refs: scatter_kernel(cols, *refs),
        out_shape=jax.ShapeDtypeStruct((rows, 3 * cols), F32),
        in_specs=[pl.BlockSpec(memory_space=pl.ANY)],
        out_specs=pl.BlockSpec(memory_space=pltpu.VMEM),
        scratch_shapes=[
            pltpu.VMEM((2, 2, 2, rows, 3 * cols), F32),
            pltpu.VMEM((2, 2, 2, rows, 3 * cols), F32),
            pltpu.VMEM((3, 2, 2, rows, cols), F32),
            pltpu.VMEM((3, 2, rows, cols), F32),
            pltpu.VMEM((3, rows, cols), F32),
            pltpu.SemaphoreType.DMA,
            pltpu.SemaphoreType.DMA((27,)),
            pltpu.SemaphoreType.DMA((27,)),
        ],
        compiler_params=pltpu.CompilerParams(collective_id=0, has_side_effects=True, vmem_limit_bytes=52 << 20),
        cost_estimate=pl.CostEstimate(flops=60 << 30, bytes_accessed=64 << 20, transcendentals=0),
        name='scatter_all',
    )(g6)


def z_pair(arr):
    return lax.ppermute(arr, AX, Z_PERM)


barrier = lax.optimization_barrier


def group_gather(arr):
    return lax.all_gather(arr, AX, axis=0, tiled=True, axis_index_groups=GROUPS)


def group_scatter(arr):
    return lax.psum_scatter(arr, AX, scatter_dimension=0, tiled=True, axis_index_groups=GROUPS)


def xor_send(arr, step):
    return lax.ppermute(arr, AX, [(i, i ^ step) for i in range(N_DEV)])


def plane_gather(arr, rank):
    n_half = arr.shape[0] // CHUNKS
    via_x, via_y = xor_send(arr, 2), xor_send(arr, 4)
    halves = {0: (arr[:n_half], arr[n_half:]), 2: (via_x[:n_half], via_x[n_half:]), 4: (via_y[:n_half], via_y[n_half:])}
    halves[6] = (xor_send(halves[4][0], 2), xor_send(halves[2][1], 4))
    own_core, x_core, y_core = xor_send(arr, 1), xor_send(via_x, 1), xor_send(via_y, 1)
    for step, both in ((1, own_core), (3, x_core), (5, y_core)):
        halves[step] = (both[:n_half], both[n_half:])
    halves[7] = tuple(xor_send(part, 1) for part in halves[6])
    out = []
    for c in range(CHUNKS):
        buf = jnp.zeros((TP,) + halves[0][c].shape, BF16)
        for step in range(TP):
            buf = lax.dynamic_update_slice(buf, halves[step][c][None], (rank ^ step, 0, 0))
        out.append(buf.reshape(TP * n_half, arr.shape[1]))
    return out


def local_step(hidden, grad_out, positions, gain_attn, w_q, b_q, w_k, b_k, w_v, b_v, w_o, gain_mlp, w_gate, w_up, w_down):
    n_seq, width = hidden.shape[1], hidden.shape[2]
    rows = w_q.shape[0]
    q_width, kv_width = w_q.shape[1], w_k.shape[1]
    n_heads, n_kv = q_width // HEAD_DIM, kv_width // HEAD_DIM
    ff_blk = w_down.shape[0]
    ff_loc = 2 * ff_blk
    half = width // 2
    dev = lax.axis_index(AX)
    z_idx, rank = dev // TP, dev % TP
    z_zero = z_idx == 0
    hidden = hidden[0]
    grad_out = grad_out[0]

    kvb = jnp.concatenate([b_k, b_v, jnp.zeros((rows - 2 * b_k.shape[0],), BF16)])
    small = jnp.stack([gain_attn, b_q, gain_mlp, kvb], axis=1)
    small = jnp.pad(small, ((0, 0), (0, 124)))
    qkv_loc = jnp.concatenate([w_q, w_k, w_v, small], axis=1)
    qkv_full = lax.all_gather(qkv_loc, AX, axis=0, tiled=True)
    n_qkv = q_width + 2 * kv_width
    w_o_full = lax.all_gather(w_o, AX, axis=0, tiled=True)

    gu = cut_columns(w_gate, w_up, ff_blk)
    gu, hidden = barrier((gu, hidden))
    gu_rows = jnp.zeros((2, TP, rows, ff_loc), BF16)
    for d in range(TP):
        piece = lax.dynamic_index_in_dim(gu, rank ^ d, 0, keepdims=False)
        if d:
            piece = lax.ppermute(piece, AX, [(i, i ^ d) for i in range(N_DEV)])
        gu_rows = lax.dynamic_update_slice(gu_rows, piece[:, None], (0, rank ^ d, 0, 0))
    gu_rows = gu_rows.reshape(2, half, ff_loc)

    w_qkv = qkv_full[:, :n_qkv]
    small_t = qkv_full[:, n_qkv:n_qkv + 4].T.astype(F32)
    gain_a, bias_q, gain_m = small_t[0], small_t[1], small_t[2]
    kvb_full = small_t[3].reshape(N_DEV, rows)
    n_b = b_k.shape[0]
    bias = jnp.concatenate([bias_q, kvb_full[:, :n_b].reshape(kv_width), kvb_full[:, n_b:2 * n_b].reshape(kv_width)])
    cos_t, sin_t = rope_tables(positions[0])
    normed_attn, inv_attn = norm_fwd(hidden, gain_a)
    qkv = dot('sd,de->se', normed_attn, w_qkv) + bias
    qkv, gu_rows, grad_out, w_down = barrier((qkv, gu_rows, grad_out, w_down))
    gu_other = z_pair(gu_rows)
    down_other = z_pair(w_down)
    go_all = plane_gather(grad_out, rank)
    attn_out = attn_fwd(qkv, cos_t, sin_t, n_heads, n_kv)
    resid_mid = (hidden.astype(F32) + dot('se,ed->sd', attn_out, w_o_full)).astype(BF16)
    normed_mlp, inv_mlp = norm_fwd(resid_mid, gain_m)
    n_ch = n_seq // CHUNKS
    h_all = [group_gather(normed_mlp[c * n_ch:(c + 1) * n_ch]) for c in range(CHUNKS)]

    gu_lo = jnp.where(z_zero, gu_rows, gu_other)
    gu_hi = jnp.where(z_zero, gu_other, gu_rows)
    w_g = jnp.concatenate([gu_lo[0], gu_hi[0]], axis=0)
    w_u = jnp.concatenate([gu_lo[1], gu_hi[1]], axis=0)
    w_d = jnp.concatenate([jnp.where(z_zero, w_down, down_other), jnp.where(z_zero, down_other, w_down)], axis=0)

    pre = []
    for c in range(CHUNKS):
        gate_pre = dot('sd,df->sf', h_all[c], w_g)
        up_proj = dot('sd,df->sf', h_all[c], w_u)
        pre.append((gate_pre, up_proj))
    acts, d_gates, d_ups, dn_sums = [], [], [], []
    for c in range(CHUNKS):
        gate_pre, up_proj = pre[c]
        act = (jax.nn.silu(gate_pre) * up_proj).astype(BF16)
        d_act = dot('sd,fd->sf', go_all[c], w_d).astype(BF16).astype(F32)
        gate_sig = jax.nn.sigmoid(gate_pre)
        d_gate = (d_act * up_proj * gate_sig * (1.0 + gate_pre * (1.0 - gate_sig))).astype(BF16)
        d_up = (d_act * gate_pre * gate_sig).astype(BF16)
        dn_part = dot('sf,df->sd', d_gate, w_g) + dot('sf,df->sd', d_up, w_u)
        dn_sums.append(group_scatter(dn_part))
        acts.append(act)
        d_gates.append(d_gate)
        d_ups.append(d_up)
    dn_part, acts, d_gates, d_ups, h_all = barrier((dn_part, acts, d_gates, d_ups, h_all))

    def token_dot(eq_form, lhs_list, rhs_list):
        total = dot(eq_form, lhs_list[0], rhs_list[0])
        for lhs, rhs in zip(lhs_list[1:], rhs_list[1:]):
            total = total + dot(eq_form, lhs, rhs)
        return total

    h_send = [lax.dynamic_slice_in_dim(h, (1 - z_idx) * half, half, axis=1) for h in h_all]
    h_keep = [lax.dynamic_slice_in_dim(h, z_idx * half, half, axis=1) for h in h_all]
    gg_send = token_dot('sd,sf->df', h_send, d_gates)
    gu_send = token_dot('sd,sf->df', h_send, d_ups)
    d_wd = token_dot('sf,sd->fd', acts, go_all)
    wd_send = lax.dynamic_slice_in_dim(d_wd, (1 - z_idx) * ff_blk, ff_blk, axis=0)
    wd_keep = lax.dynamic_slice_in_dim(d_wd, z_idx * ff_blk, ff_blk, axis=0)
    gg_recv, gu_recv, wd_recv = z_pair(gg_send), z_pair(gu_send), z_pair(wd_send)
    gg_keep = token_dot('sd,sf->df', h_keep, d_gates)
    gu_keep = token_dot('sd,sf->df', h_keep, d_ups)
    out_part = [dot('sf,fd->sd', act, w_d) for act in acts]
    dn_sums, gg_keep, gu_keep, out_part, wd_keep = barrier((dn_sums, gg_keep, gu_keep, out_part, wd_keep))
    d_normed_mlp = jnp.concatenate(dn_sums, axis=0).astype(BF16).astype(F32)
    out_sum = jnp.concatenate([group_scatter(part) for part in out_part], axis=0)

    def back_rows(grad):
        grad = lax.all_to_all(grad.reshape(TP, rows, ff_loc), AX, 0, 0, axis_index_groups=GROUPS, tiled=True)
        return join_columns(grad, ff_blk)

    g_w_up = back_rows(gu_keep + gu_recv)

    d_resid_norm, d_gain_m = norm_bwd(resid_mid, inv_mlp, gain_m, d_normed_mlp)
    d_resid = (grad_out.astype(F32) + d_resid_norm).astype(BF16)
    d_attn = dot('sd,ed->se', d_resid, w_o_full).astype(BF16)
    d_q, d_k, d_v, d_b_q, d_b_k, d_b_v = attn_bwd(qkv, d_attn, cos_t, sin_t, n_heads, n_kv)
    gg_keep, _ = barrier((gg_keep, d_b_k))
    g_w_gate = back_rows(gg_keep + gg_recv)
    d_qkv = jnp.concatenate([d_q, d_k, d_v], axis=1)
    d_normed_attn = dot('se,de->sd', d_qkv, w_qkv).astype(BF16).astype(F32)
    d_hidden_norm, d_gain_a = norm_bwd(hidden, inv_attn, gain_a, d_normed_attn)
    grad_hidden = (d_resid.astype(F32) + d_hidden_norm).astype(BF16)

    d_kvb = jnp.concatenate([d_b_k.reshape(N_DEV, n_b), d_b_v.reshape(N_DEV, n_b), jnp.zeros((N_DEV, rows - 2 * n_b), F32)], axis=1)
    d_small = jnp.stack([d_gain_a, d_b_q[0], d_gain_m, d_kvb.reshape(width)], axis=1)
    d_small = jnp.pad(d_small, ((0, 0), (0, GRAD_BLK - 4)))
    grads = attn_grads(attn_out.T, d_resid, normed_attn.T, d_qkv, d_small)
    grads = scatter_all(grads, rows)
    out_sum, wd_keep, grads = barrier((out_sum, wd_keep, grads))
    g_w_down = wd_keep + wd_recv
    layer_out = (resid_mid.astype(F32) + out_sum).astype(BF16)
    g_w_o, g_qkv = grads[:, :width], grads[:, width:]
    g_w_q = g_qkv[:, :q_width]
    g_w_k = g_qkv[:, q_width:q_width + kv_width]
    g_w_v = g_qkv[:, q_width + kv_width:n_qkv]
    g_small = g_qkv[:, n_qkv:n_qkv + 4].T
    g_kvb = g_small[3]
    return (layer_out[None], grad_hidden[None], g_small[0], g_w_q, g_small[1], g_w_k, g_kvb[:n_b], g_w_v, g_kvb[n_b:2 * n_b],
            g_w_o, g_small[2], g_w_gate, g_w_up, g_w_down)


def solution(mesh):
    act_spec = P(AX, None, None)
    mat_spec = P(AX, None)
    vec_spec = P(AX)
    param_specs = (vec_spec, mat_spec, vec_spec, mat_spec, vec_spec, mat_spec, vec_spec, mat_spec, vec_spec, mat_spec, mat_spec, mat_spec)
    in_specs_all = (act_spec, act_spec, mat_spec) + param_specs
    out_specs_all = (act_spec, act_spec) + param_specs

    return jax.shard_map(local_step, mesh=mesh, in_specs=in_specs_all, out_specs=out_specs_all, check_vma=False)
```

```python
import math
import jax
import jax.numpy as jnp
from jax import lax
from jax.experimental import pallas as pl
from jax.experimental.pallas import tpu as pltpu
from jax.sharding import PartitionSpec as P

HEAD_DIM = 128
NORM_EPS = 1e-6
ROPE_THETA = 1000000.0
AX = 'fsdp'
N_DEV = 16
TP = 8
GROUPS = [list(range(0, 8)), list(range(8, 16))]
Z_PERM = [(i, i ^ 8) for i in range(N_DEV)]
F32 = jnp.float32
BF16 = jnp.bfloat16
CHUNKS = 2


def dot(eq_form, lhs_arr, rhs_arr):
    return jnp.einsum(eq_form, lhs_arr, rhs_arr, preferred_element_type=F32)


def rope_tables(positions):
    inv_freq = 1.0 / jnp.power(ROPE_THETA, jnp.arange(0, HEAD_DIM, 2).astype(F32) / HEAD_DIM)
    angles = positions.astype(F32)[:, None] * inv_freq
    cos_h, sin_h = jnp.cos(angles), jnp.sin(angles)
    return jnp.concatenate([cos_h, cos_h], axis=-1), jnp.concatenate([-sin_h, sin_h], axis=-1)


def rope(vec, cos_t, sin_t):
    return vec * cos_t + pltpu.roll(vec, HEAD_DIM // 2, 1) * sin_t


def rope_t(vec, cos_t, sin_t):
    return vec * cos_t - pltpu.roll(vec, HEAD_DIM // 2, 1) * sin_t


def dot_nt(lhs, rhs):
    return lax.dot_general(lhs, rhs, (((1,), (1,)), ((), ())), preferred_element_type=F32)


def dot_nn(lhs, rhs):
    return lax.dot_general(lhs, rhs, (((1,), (0,)), ((), ())), preferred_element_type=F32)


def dot_tn(lhs, rhs):
    return lax.dot_general(lhs, rhs, (((0,), (0,)), ((), ())), preferred_element_type=F32)


SCALE = 1.0 / math.sqrt(HEAD_DIM)


def attn_fwd_kernel(q_ref, k_ref, v_ref, cos_ref, sin_ref, o_ref):
    cos_t, sin_t = cos_ref[...], sin_ref[...]
    q_rot = rope(q_ref[...], cos_t, sin_t).astype(BF16)
    k_rot = rope(k_ref[...], cos_t, sin_t).astype(BF16)
    scores = dot_nt(q_rot, k_rot) * SCALE
    keep = lax.broadcasted_iota(jnp.int32, scores.shape, 0) >= lax.broadcasted_iota(jnp.int32, scores.shape, 1)
    scores = jnp.where(keep, scores, -1e30)
    probs = jnp.exp(scores - jnp.max(scores, axis=1, keepdims=True))
    probs = probs * (1.0 / jnp.sum(probs, axis=1, keepdims=True))
    o_ref[...] = dot_nn(probs.astype(BF16), v_ref[...].astype(BF16)).astype(BF16)


def attn_fwd(qkv, cos_t, sin_t, n_heads, n_kv):
    n_seq = qkv.shape[0]
    group = n_heads // n_kv
    tab = pl.BlockSpec((n_seq, HEAD_DIM), lambda h: (0, 0))
    return pl.pallas_call(
        attn_fwd_kernel,
        grid=(n_heads,),
        in_specs=[
            pl.BlockSpec((n_seq, HEAD_DIM), lambda h: (0, h)),
            pl.BlockSpec((n_seq, HEAD_DIM), lambda h: (0, n_heads + h // group)),
            pl.BlockSpec((n_seq, HEAD_DIM), lambda h: (0, n_heads + n_kv + h // group)),
            tab, tab,
        ],
        out_specs=pl.BlockSpec((n_seq, HEAD_DIM), lambda h: (0, h)),
        out_shape=jax.ShapeDtypeStruct((n_seq, n_heads * HEAD_DIM), BF16),
        compiler_params=pltpu.CompilerParams(vmem_limit_bytes=40 << 20),
        cost_estimate=pl.CostEstimate(flops=8 << 30, bytes_accessed=6 << 20, transcendentals=3 << 20),
        name='attn_fwd',
    )(qkv, qkv, qkv, cos_t, sin_t)


def attn_bwd_kernel(q_ref, k_ref, v_ref, do_ref, cos_ref, sin_ref, dq_ref, dk_ref, dv_ref, bq_ref, bk_ref, bv_ref, dk_acc, dv_acc):
    step = pl.program_id(1)
    cos_t, sin_t = cos_ref[...], sin_ref[...]
    q_rot = rope(q_ref[...], cos_t, sin_t).astype(BF16)
    k_rot = rope(k_ref[...], cos_t, sin_t).astype(BF16)
    v_st = v_ref[...].astype(BF16)
    d_out = do_ref[...]
    scores = dot_nt(k_rot, q_rot) * SCALE
    keep = lax.broadcasted_iota(jnp.int32, scores.shape, 1) >= lax.broadcasted_iota(jnp.int32, scores.shape, 0)
    scores = jnp.where(keep, scores, -1e30)
    probs = jnp.exp(scores - jnp.max(scores, axis=0, keepdims=True))
    probs = probs * (1.0 / jnp.sum(probs, axis=0, keepdims=True))
    d_v = dot_nn(probs.astype(BF16), d_out)
    d_probs = dot_nt(v_st, d_out)
    d_sc = (probs * (d_probs - jnp.sum(probs * d_probs, axis=0, keepdims=True)) * SCALE).astype(BF16)
    d_k = dot_nn(d_sc, q_rot)
    d_q = dot_tn(d_sc, k_rot).astype(BF16).astype(F32)
    d_q = rope_t(d_q, cos_t, sin_t)
    dq_ref[...] = d_q.astype(BF16)
    bq_ref[...] = jnp.sum(d_q, axis=0, keepdims=True)

    @pl.when(step == 0)
    def _():
        dk_acc[...] = d_k
        dv_acc[...] = d_v

    @pl.when(step > 0)
    def _():
        dk_acc[...] += d_k
        dv_acc[...] += d_v

    @pl.when(step == pl.num_programs(1) - 1)
    def _():
        d_k_all = rope_t(dk_acc[...].astype(BF16).astype(F32), cos_t, sin_t)
        dk_ref[...] = d_k_all.astype(BF16)
        bk_ref[...] = jnp.sum(d_k_all, axis=0, keepdims=True)
        d_v_all = dv_acc[...].astype(BF16)
        dv_ref[...] = d_v_all
        bv_ref[...] = jnp.sum(d_v_all.astype(F32), axis=0, keepdims=True)


def attn_bwd(qkv, d_attn, cos_t, sin_t, n_heads, n_kv):
    n_seq = qkv.shape[0]
    group = n_heads // n_kv
    tab = pl.BlockSpec((n_seq, HEAD_DIM), lambda j, g: (0, 0))
    blk_h = pl.BlockSpec((n_seq, HEAD_DIM), lambda j, g: (0, j * group + g))
    blk_kv = pl.BlockSpec((n_seq, HEAD_DIM), lambda j, g: (0, j))
    vec_h = pl.BlockSpec((1, HEAD_DIM), lambda j, g: (0, j * group + g))
    vec_kv = pl.BlockSpec((1, HEAD_DIM), lambda j, g: (0, j))
    q_width, kv_width = n_heads * HEAD_DIM, n_kv * HEAD_DIM
    return pl.pallas_call(
        attn_bwd_kernel,
        grid=(n_kv, group),
        in_specs=[
            blk_h,
            pl.BlockSpec((n_seq, HEAD_DIM), lambda j, g: (0, n_heads + j)),
            pl.BlockSpec((n_seq, HEAD_DIM), lambda j, g: (0, n_heads + n_kv + j)),
            blk_h, tab, tab,
        ],
        out_specs=[blk_h, blk_kv, blk_kv, vec_h, vec_kv, vec_kv],
        out_shape=[
            jax.ShapeDtypeStruct((n_seq, q_width), BF16),
            jax.ShapeDtypeStruct((n_seq, kv_width), BF16),
            jax.ShapeDtypeStruct((n_seq, kv_width), BF16),
            jax.ShapeDtypeStruct((1, q_width), F32),
            jax.ShapeDtypeStruct((1, kv_width), F32),
            jax.ShapeDtypeStruct((1, kv_width), F32),
        ],
        scratch_shapes=[pltpu.VMEM((n_seq, HEAD_DIM), F32), pltpu.VMEM((n_seq, HEAD_DIM), F32)],
        compiler_params=pltpu.CompilerParams(vmem_limit_bytes=40 << 20),
        cost_estimate=pl.CostEstimate(flops=16 << 30, bytes_accessed=10 << 20, transcendentals=3 << 20),
        name='attn_bwd',
    )(qkv, qkv, qkv, d_attn, cos_t, sin_t)


GRAD_BLK = 256


def attn_grads_kernel(n_o, n_all, lhs_o_ref, lhs_h_ref, rhs_o_ref, rhs_h_ref, small_ref, out_ref):
    step = pl.program_id(0)

    @pl.when(step < n_o)
    def _():
        out_ref[...] = dot_nn(lhs_o_ref[...], rhs_o_ref[...])

    @pl.when(jnp.logical_and(step >= n_o, step < n_all))
    def _():
        out_ref[...] = dot_nn(lhs_h_ref[...], rhs_h_ref[...])

    @pl.when(step == n_all)
    def _():
        out_ref[...] = small_ref[...]


def attn_grads(lhs_o, rhs_o, lhs_h, rhs_h, small):
    width, n_seq = lhs_o.shape
    n_o, n_h = rhs_o.shape[1] // GRAD_BLK, rhs_h.shape[1] // GRAD_BLK
    n_all = n_o + n_h
    full = pl.BlockSpec((width, n_seq), lambda j: (0, 0))
    return pl.pallas_call(
        lambda *refs: attn_grads_kernel(n_o, n_all, *refs),
        grid=(n_all + 1,),
        in_specs=[
            full, full,
            pl.BlockSpec((n_seq, GRAD_BLK), lambda j: (0, jnp.minimum(j, n_o - 1))),
            pl.BlockSpec((n_seq, GRAD_BLK), lambda j: (0, jnp.clip(j - n_o, 0, n_h - 1))),
            pl.BlockSpec((width, GRAD_BLK), lambda j: (0, 0)),
        ],
        out_specs=pl.BlockSpec((width, GRAD_BLK), lambda j: (0, j)),
        out_shape=jax.ShapeDtypeStruct((width, (n_all + 1) * GRAD_BLK), F32),
        compiler_params=pltpu.CompilerParams(vmem_limit_bytes=40 << 20),
        cost_estimate=pl.CostEstimate(flops=12 << 30, bytes_accessed=32 << 20, transcendentals=0),
        name='attn_grads',
    )(lhs_o, lhs_h, rhs_o, rhs_h, small)


def norm_fwd(hidden, gain_vec):
    x_f32 = hidden.astype(F32)
    inv_rms = lax.rsqrt(jnp.mean(x_f32 * x_f32, axis=-1, keepdims=True) + NORM_EPS)
    return (x_f32 * inv_rms * gain_vec).astype(BF16), inv_rms


def norm_bwd(hidden, inv_rms, gain_vec, d_normed):
    unit_rows = hidden.astype(F32) * inv_rms
    d_gain = jnp.sum(d_normed * unit_rows, axis=0)
    d_unit = d_normed * gain_vec
    d_hidden = inv_rms * (d_unit - unit_rows * jnp.mean(d_unit * unit_rows, axis=-1, keepdims=True))
    return d_hidden, d_gain


def cut_kernel(blk, n_rank, gate_ref, up_ref, out_ref):
    for r in range(n_rank):
        for g, src in enumerate((gate_ref, up_ref)):
            out_ref[r, g, :, 0:blk] = src[:, r * blk:(r + 1) * blk]
            out_ref[r, g, :, blk:2 * blk] = src[:, (n_rank + r) * blk:(n_rank + r + 1) * blk]


def cut_columns(w_gate, w_up, blk):
    rows = w_gate.shape[0]
    return pl.pallas_call(
        lambda *refs: cut_kernel(blk, TP, *refs),
        out_shape=jax.ShapeDtypeStruct((TP, 2, rows, 2 * blk), BF16),
        in_specs=[pl.BlockSpec(memory_space=pltpu.VMEM)] * 2,
        out_specs=pl.BlockSpec(memory_space=pltpu.VMEM),
        compiler_params=pltpu.CompilerParams(vmem_limit_bytes=24 << 20),
        cost_estimate=pl.CostEstimate(flops=4 << 30, bytes_accessed=8 << 20, transcendentals=0),
        name='cut_columns',
    )(w_gate, w_up)


def join_kernel(blk, n_rank, src_ref, out_ref):
    for r in range(n_rank):
        out_ref[:, r * blk:(r + 1) * blk] = src_ref[r, :, 0:blk]
        out_ref[:, (n_rank + r) * blk:(n_rank + r + 1) * blk] = src_ref[r, :, blk:2 * blk]


def join_columns(parts, blk):
    rows = parts.shape[1]
    tile = 32
    return pl.pallas_call(
        lambda *refs: join_kernel(blk, TP, *refs),
        grid=(rows // tile,),
        out_shape=jax.ShapeDtypeStruct((rows, 2 * TP * blk), F32),
        in_specs=[pl.BlockSpec((TP, tile, 2 * blk), lambda i: (0, i, 0))],
        out_specs=pl.BlockSpec((tile, 2 * TP * blk), lambda i: (i, 0)),
        compiler_params=pltpu.CompilerParams(vmem_limit_bytes=24 << 20),
        cost_estimate=pl.CostEstimate(flops=4 << 30, bytes_accessed=8 << 20, transcendentals=0),
        name='join_columns',
    )(parts)


def scatter_kernel(cols, g_ref, out_ref, own, from_core, buf1, buf2, buf3, load_sem, send_sem, recv_sem):
    dev = lax.axis_index(AX)
    me = (dev // 8, (dev // 4) % 2, (dev // 2) % 2)
    core = dev % 2
    peer_core = dev + 1 - 2 * core
    peers = tuple(dev + step * (1 - 2 * pos) for step, pos in zip((8, 4, 2), me))
    barrier_sem = pltpu.get_barrier_semaphore()
    for peer in (peer_core,) + peers:
        pl.semaphore_signal(barrier_sem, inc=1, device_id=(peer,), device_id_type=pl.DeviceIdType.MESH)
    pl.semaphore_wait(barrier_sem, 4)
    orders = ((2, 1, 0), (1, 0, 2), (0, 2, 1))
    load = pltpu.make_async_copy(g_ref.at[:, :, :, core], own, load_sem)
    load.start()

    def pick(fixed):
        return tuple(fixed.get(d, slice(None)) for d in range(3))

    def remote(slot, src, dst, peer):
        copy = pltpu.make_async_remote_copy(
            src_ref=src, dst_ref=dst, send_sem=send_sem.at[slot], recv_sem=recv_sem.at[slot],
            device_id=(peer,), device_id_type=pl.DeviceIdType.MESH)
        copy.start()
        return copy

    def col(k):
        return pl.ds(k * cols, cols)

    core_copies = {}
    for half in range(2):
        for k, order in enumerate(orders):
            where = pick({order[0]: me[order[0]] if half else 1 - me[order[0]]})
            core_copies[half, k] = remote(
                half * 3 + k, g_ref.at[where + (1 - core, slice(None), col(k))],
                from_core.at[where + (slice(None), col(k))], peer_core)
    load.wait()

    def add(dst, src, count):
        def body(i, carry):
            a, b = i // 2, i % 2
            dst(a, b)[...] = dst(a, b)[...] + src(a, b)[...]
            return carry

        lax.fori_loop(0, count, body, 0)

    def at4(ref, k, order, first):
        def get(a, b):
            fixed = {order[0]: first, order[1]: a, order[2]: b}
            return ref.at[tuple(fixed[d] for d in range(3)) + (slice(None), col(k))]

        return get

    def at2(ref, k, order, second):
        def get(a, b):
            fixed = {order[0]: me[order[0]], order[1]: second, order[2]: b}
            return ref.at[tuple(fixed[d] for d in range(3)) + (slice(None), col(k))]

        return get

    stage1, stage2, stage3 = {}, {}, {}
    for k, order in enumerate(orders):
        core_copies[0, k].wait_recv()
        far = 1 - me[order[0]]
        add(at4(own, k, order, far), at4(from_core, k, order, far), 4)
    for k, order in enumerate(orders):
        for a in range(2):
            for b in range(2):
                fixed = {order[0]: 1 - me[order[0]], order[1]: a, order[2]: b}
                src = own.at[tuple(fixed[d] for d in range(3)) + (slice(None), col(k))]
                stage1[k, a, b] = remote(6 + k * 4 + a * 2 + b, src, buf1.at[k, a, b], peers[order[0]])
    for k, order in enumerate(orders):
        core_copies[1, k].wait_recv()
        near = me[order[0]]
        add(at4(own, k, order, near), at4(from_core, k, order, near), 4)
    for k, order in enumerate(orders):
        for a in range(2):
            for b in range(2):
                stage1[k, a, b].wait_recv()
        add(at4(own, k, order, me[order[0]]), lambda a, b, k=k: buf1.at[k, a, b], 4)
    for k, order in enumerate(orders):
        for b in range(2):
            src = at2(own, k, order, 1 - me[order[1]])(0, b)
            stage2[k, b] = remote(18 + k * 2 + b, src, buf2.at[k, b], peers[order[1]])
    for k, order in enumerate(orders):
        for b in range(2):
            stage2[k, b].wait_recv()
        add(at2(own, k, order, me[order[1]]), lambda a, b, k=k: buf2.at[k, b], 2)
    for k, order in enumerate(orders):
        src = at2(own, k, order, me[order[1]])(0, 1 - me[order[2]])
        stage3[k] = remote(24 + k, src, buf3.at[k], peers[order[2]])
    for k, order in enumerate(orders):
        stage3[k].wait_recv()
        out_ref[:, k * cols:(k + 1) * cols] = at2(own, k, order, me[order[1]])(0, me[order[2]])[...] + buf3[k]
    for copy in list(core_copies.values()) + list(stage1.values()) + list(stage2.values()) + list(stage3.values()):
        copy.wait_send()


def scatter_all(grads, rows):
    cols = grads.shape[1] // 3
    g6 = grads.reshape(2, 2, 2, 2, rows, 3 * cols)
    return pl.pallas_call(
        lambda *refs: scatter_kernel(cols, *refs),
        out_shape=jax.ShapeDtypeStruct((rows, 3 * cols), F32),
        in_specs=[pl.BlockSpec(memory_space=pl.ANY)],
        out_specs=pl.BlockSpec(memory_space=pltpu.VMEM),
        scratch_shapes=[
            pltpu.VMEM((2, 2, 2, rows, 3 * cols), F32),
            pltpu.VMEM((2, 2, 2, rows, 3 * cols), F32),
            pltpu.VMEM((3, 2, 2, rows, cols), F32),
            pltpu.VMEM((3, 2, rows, cols), F32),
            pltpu.VMEM((3, rows, cols), F32),
            pltpu.SemaphoreType.DMA,
            pltpu.SemaphoreType.DMA((27,)),
            pltpu.SemaphoreType.DMA((27,)),
        ],
        compiler_params=pltpu.CompilerParams(collective_id=0, has_side_effects=True, vmem_limit_bytes=52 << 20),
        cost_estimate=pl.CostEstimate(flops=60 << 30, bytes_accessed=64 << 20, transcendentals=0),
        name='scatter_all',
    )(g6)


def z_pair(arr):
    return lax.ppermute(arr, AX, Z_PERM)


barrier = lax.optimization_barrier


def group_gather(arr):
    return lax.all_gather(arr, AX, axis=0, tiled=True, axis_index_groups=GROUPS)


def group_scatter(arr):
    return lax.psum_scatter(arr, AX, scatter_dimension=0, tiled=True, axis_index_groups=GROUPS)


def xor_send(arr, step):
    return lax.ppermute(arr, AX, [(i, i ^ step) for i in range(N_DEV)])


def plane_gather(arr, rank):
    n_half = arr.shape[0] // CHUNKS
    via_x, via_y = xor_send(arr, 2), xor_send(arr, 4)
    halves = {0: (arr[:n_half], arr[n_half:]), 2: (via_x[:n_half], via_x[n_half:]), 4: (via_y[:n_half], via_y[n_half:])}
    halves[6] = (xor_send(halves[4][0], 2), xor_send(halves[2][1], 4))
    own_core, x_core, y_core = xor_send(arr, 1), xor_send(via_x, 1), xor_send(via_y, 1)
    for step, both in ((1, own_core), (3, x_core), (5, y_core)):
        halves[step] = (both[:n_half], both[n_half:])
    halves[7] = tuple(xor_send(part, 1) for part in halves[6])
    out = []
    for c in range(CHUNKS):
        buf = jnp.zeros((TP,) + halves[0][c].shape, BF16)
        for step in range(TP):
            buf = lax.dynamic_update_slice(buf, halves[step][c][None], (rank ^ step, 0, 0))
        out.append(buf.reshape(TP * n_half, arr.shape[1]))
    return out


def local_step(hidden, grad_out, positions, gain_attn, w_q, b_q, w_k, b_k, w_v, b_v, w_o, gain_mlp, w_gate, w_up, w_down):
    n_seq, width = hidden.shape[1], hidden.shape[2]
    rows = w_q.shape[0]
    q_width, kv_width = w_q.shape[1], w_k.shape[1]
    n_heads, n_kv = q_width // HEAD_DIM, kv_width // HEAD_DIM
    ff_blk = w_down.shape[0]
    ff_loc = 2 * ff_blk
    half = width // 2
    dev = lax.axis_index(AX)
    z_idx, rank = dev // TP, dev % TP
    z_zero = z_idx == 0
    hidden = hidden[0]
    grad_out = grad_out[0]

    kvb = jnp.concatenate([b_k, b_v, jnp.zeros((rows - 2 * b_k.shape[0],), BF16)])
    small = jnp.stack([gain_attn, b_q, gain_mlp, kvb], axis=1)
    small = jnp.pad(small, ((0, 0), (0, 124)))
    qkv_loc = jnp.concatenate([w_q, w_k, w_v, small], axis=1)
    qkv_full = lax.all_gather(qkv_loc, AX, axis=0, tiled=True)
    n_qkv = q_width + 2 * kv_width
    w_o_full = lax.all_gather(w_o, AX, axis=0, tiled=True)

    gu = cut_columns(w_gate, w_up, ff_blk)
    gu, hidden = barrier((gu, hidden))
    own_rows, other_rows = [], []
    for g in range(2):
        buf = jnp.zeros((TP, rows, ff_loc), BF16)
        for d in range(TP):
            piece = lax.dynamic_slice(gu, (rank ^ d, g, 0, 0), (1, 1, rows, ff_loc))[:, 0]
            if d:
                piece = lax.ppermute(piece, AX, [(i, i ^ d) for i in range(N_DEV)])
            buf = lax.dynamic_update_slice(buf, piece, (rank ^ d, 0, 0))
        buf = buf.reshape(half, ff_loc)
        own_rows.append(buf)
        other_rows.append(z_pair(buf))
    down_other = z_pair(w_down)

    w_qkv = qkv_full[:, :n_qkv]
    small_t = qkv_full[:, n_qkv:n_qkv + 4].T.astype(F32)
    gain_a, bias_q, gain_m = small_t[0], small_t[1], small_t[2]
    kvb_full = small_t[3].reshape(N_DEV, rows)
    n_b = b_k.shape[0]
    bias = jnp.concatenate([bias_q, kvb_full[:, :n_b].reshape(kv_width), kvb_full[:, n_b:2 * n_b].reshape(kv_width)])
    cos_t, sin_t = rope_tables(positions[0])
    normed_attn, inv_attn = norm_fwd(hidden, gain_a)
    qkv = dot('sd,de->se', normed_attn, w_qkv) + bias
    qkv, grad_out = barrier((qkv, grad_out))
    go_all = plane_gather(grad_out, rank)
    attn_out = attn_fwd(qkv, cos_t, sin_t, n_heads, n_kv)
    resid_mid = (hidden.astype(F32) + dot('se,ed->sd', attn_out, w_o_full)).astype(BF16)
    normed_mlp, inv_mlp = norm_fwd(resid_mid, gain_m)
    n_ch = n_seq // CHUNKS
    h_all = [group_gather(normed_mlp[c * n_ch:(c + 1) * n_ch]) for c in range(CHUNKS)]

    def z_order(own, other):
        return jnp.concatenate([jnp.where(z_zero, own, other), jnp.where(z_zero, other, own)], axis=0)

    w_g, w_u = z_order(own_rows[0], other_rows[0]), z_order(own_rows[1], other_rows[1])
    w_d = z_order(w_down, down_other)

    pre = []
    for c in range(CHUNKS):
        gate_pre = dot('sd,df->sf', h_all[c], w_g)
        up_proj = dot('sd,df->sf', h_all[c], w_u)
        pre.append((gate_pre, up_proj))
    acts, d_gates, d_ups, dn_sums = [], [], [], []
    gate_pre, up_proj = pre[0]
    act_first = (jax.nn.silu(gate_pre) * up_proj).astype(BF16)
    out_first = dot('sf,fd->sd', act_first, w_d)
    out_first, go_all[0] = barrier((out_first, go_all[0]))
    out_sums = [group_scatter(out_first)]
    for c in range(CHUNKS):
        gate_pre, up_proj = pre[c]
        act = act_first if c == 0 else (jax.nn.silu(gate_pre) * up_proj).astype(BF16)
        d_act = dot('sd,fd->sf', go_all[c], w_d).astype(BF16).astype(F32)
        gate_sig = jax.nn.sigmoid(gate_pre)
        d_gate = (d_act * up_proj * gate_sig * (1.0 + gate_pre * (1.0 - gate_sig))).astype(BF16)
        d_up = (d_act * gate_pre * gate_sig).astype(BF16)
        dn_part = dot('sf,df->sd', d_gate, w_g) + dot('sf,df->sd', d_up, w_u)
        dn_sums.append(group_scatter(dn_part))
        acts.append(act)
        d_gates.append(d_gate)
        d_ups.append(d_up)
    dn_part, acts, d_gates, d_ups, h_all = barrier((dn_part, acts, d_gates, d_ups, h_all))

    def token_dot(eq_form, lhs_list, rhs_list):
        total = dot(eq_form, lhs_list[0], rhs_list[0])
        for lhs, rhs in zip(lhs_list[1:], rhs_list[1:]):
            total = total + dot(eq_form, lhs, rhs)
        return total

    h_send = [lax.dynamic_slice_in_dim(h, (1 - z_idx) * half, half, axis=1) for h in h_all]
    h_keep = [lax.dynamic_slice_in_dim(h, z_idx * half, half, axis=1) for h in h_all]
    gg_send = token_dot('sd,sf->df', h_send, d_gates)
    gu_send = token_dot('sd,sf->df', h_send, d_ups)
    d_wd = token_dot('sf,sd->fd', acts, go_all)
    wd_send = lax.dynamic_slice_in_dim(d_wd, (1 - z_idx) * ff_blk, ff_blk, axis=0)
    wd_keep = lax.dynamic_slice_in_dim(d_wd, z_idx * ff_blk, ff_blk, axis=0)
    gg_recv, gu_recv, wd_recv = z_pair(gg_send), z_pair(gu_send), z_pair(wd_send)
    gg_keep = token_dot('sd,sf->df', h_keep, d_gates)
    gu_keep = token_dot('sd,sf->df', h_keep, d_ups)
    out_part = [dot('sf,fd->sd', act, w_d) for act in acts[1:]]
    gu_sum = gu_keep + gu_recv
    dn_sums, gg_keep, gu_sum, out_part, wd_keep = barrier((dn_sums, gg_keep, gu_sum, out_part, wd_keep))
    d_normed_mlp = jnp.concatenate(dn_sums, axis=0).astype(BF16).astype(F32)
    out_sum = jnp.concatenate(out_sums + [group_scatter(part) for part in out_part], axis=0)

    def back_rows(grad):
        grad = lax.all_to_all(grad.reshape(TP, rows, ff_loc), AX, 0, 0, axis_index_groups=GROUPS, tiled=True)
        return grad

    up_parts = back_rows(gu_sum)
    g_w_up = join_columns(up_parts, ff_blk)

    d_resid_norm, d_gain_m = norm_bwd(resid_mid, inv_mlp, gain_m, d_normed_mlp)
    d_resid = (grad_out.astype(F32) + d_resid_norm).astype(BF16)
    d_attn = dot('sd,ed->se', d_resid, w_o_full).astype(BF16)
    d_q, d_k, d_v, d_b_q, d_b_k, d_b_v = attn_bwd(qkv, d_attn, cos_t, sin_t, n_heads, n_kv)
    gg_keep, _, _ = barrier((gg_keep, d_b_k, up_parts))
    g_w_gate = join_columns(back_rows(gg_keep + gg_recv), ff_blk)
    d_qkv = jnp.concatenate([d_q, d_k, d_v], axis=1)
    d_normed_attn = dot('se,de->sd', d_qkv, w_qkv).astype(BF16).astype(F32)
    d_hidden_norm, d_gain_a = norm_bwd(hidden, inv_attn, gain_a, d_normed_attn)
    grad_hidden = (d_resid.astype(F32) + d_hidden_norm).astype(BF16)

    d_kvb = jnp.concatenate([d_b_k.reshape(N_DEV, n_b), d_b_v.reshape(N_DEV, n_b), jnp.zeros((N_DEV, rows - 2 * n_b), F32)], axis=1)
    d_small = jnp.stack([d_gain_a, d_b_q[0], d_gain_m, d_kvb.reshape(width)], axis=1)
    d_small = jnp.pad(d_small, ((0, 0), (0, GRAD_BLK - 4)))
    grads = attn_grads(attn_out.T, d_resid, normed_attn.T, d_qkv, d_small)
    grads = scatter_all(grads, rows)
    out_sum, wd_keep, grads = barrier((out_sum, wd_keep, grads))
    g_w_down = wd_keep + wd_recv
    layer_out = (resid_mid.astype(F32) + out_sum).astype(BF16)
    g_w_o, g_qkv = grads[:, :width], grads[:, width:]
    g_w_q = g_qkv[:, :q_width]
    g_w_k = g_qkv[:, q_width:q_width + kv_width]
    g_w_v = g_qkv[:, q_width + kv_width:n_qkv]
    g_small = g_qkv[:, n_qkv:n_qkv + 4].T
    g_kvb = g_small[3]
    return (layer_out[None], grad_hidden[None], g_small[0], g_w_q, g_small[1], g_w_k, g_kvb[:n_b], g_w_v, g_kvb[n_b:2 * n_b],
            g_w_o, g_small[2], g_w_gate, g_w_up, g_w_down)


def solution(mesh):
    act_spec = P(AX, None, None)
    mat_spec = P(AX, None)
    vec_spec = P(AX)
    param_specs = (vec_spec, mat_spec, vec_spec, mat_spec, vec_spec, mat_spec, vec_spec, mat_spec, vec_spec, mat_spec, mat_spec, mat_spec)
    in_specs_all = (act_spec, act_spec, mat_spec) + param_specs
    out_specs_all = (act_spec, act_spec) + param_specs

    return jax.shard_map(local_step, mesh=mesh, in_specs=in_specs_all, out_specs=out_specs_all, check_vma=False)
```

```python
import math
import jax
import jax.numpy as jnp
from jax import lax
from jax.experimental import pallas as pl
from jax.experimental.pallas import tpu as pltpu
from jax.sharding import PartitionSpec as P

HEAD_DIM = 128
NORM_EPS = 1e-6
ROPE_THETA = 1000000.0
AX = 'fsdp'
N_DEV = 16
TP = 8
GROUPS = [list(range(0, 8)), list(range(8, 16))]
Z_PERM = [(i, i ^ 8) for i in range(N_DEV)]
F32 = jnp.float32
BF16 = jnp.bfloat16
CHUNKS = 2


def dot(eq_form, lhs_arr, rhs_arr):
    return jnp.einsum(eq_form, lhs_arr, rhs_arr, preferred_element_type=F32)


def rope_tables(positions):
    inv_freq = 1.0 / jnp.power(ROPE_THETA, jnp.arange(0, HEAD_DIM, 2).astype(F32) / HEAD_DIM)
    angles = positions.astype(F32)[:, None] * inv_freq
    cos_h, sin_h = jnp.cos(angles), jnp.sin(angles)
    return jnp.concatenate([cos_h, cos_h], axis=-1), jnp.concatenate([-sin_h, sin_h], axis=-1)


def rope(vec, cos_t, sin_t):
    return vec * cos_t + pltpu.roll(vec, HEAD_DIM // 2, 1) * sin_t


def rope_t(vec, cos_t, sin_t):
    return vec * cos_t - pltpu.roll(vec, HEAD_DIM // 2, 1) * sin_t


def dot_nt(lhs, rhs):
    return lax.dot_general(lhs, rhs, (((1,), (1,)), ((), ())), preferred_element_type=F32)


def dot_nn(lhs, rhs):
    return lax.dot_general(lhs, rhs, (((1,), (0,)), ((), ())), preferred_element_type=F32)


def dot_tn(lhs, rhs):
    return lax.dot_general(lhs, rhs, (((0,), (0,)), ((), ())), preferred_element_type=F32)


SCALE = 1.0 / math.sqrt(HEAD_DIM)


def attn_fwd_kernel(q_ref, k_ref, v_ref, cos_ref, sin_ref, o_ref):
    cos_t, sin_t = cos_ref[...], sin_ref[...]
    q_rot = rope(q_ref[...], cos_t, sin_t).astype(BF16)
    k_rot = rope(k_ref[...], cos_t, sin_t).astype(BF16)
    scores = dot_nt(q_rot, k_rot) * SCALE
    keep = lax.broadcasted_iota(jnp.int32, scores.shape, 0) >= lax.broadcasted_iota(jnp.int32, scores.shape, 1)
    scores = jnp.where(keep, scores, -1e30)
    probs = jnp.exp(scores - jnp.max(scores, axis=1, keepdims=True))
    probs = probs * (1.0 / jnp.sum(probs, axis=1, keepdims=True))
    o_ref[...] = dot_nn(probs.astype(BF16), v_ref[...].astype(BF16)).astype(BF16)


def attn_fwd(qkv, cos_t, sin_t, n_heads, n_kv):
    n_seq = qkv.shape[0]
    group = n_heads // n_kv
    tab = pl.BlockSpec((n_seq, HEAD_DIM), lambda h: (0, 0))
    return pl.pallas_call(
        attn_fwd_kernel,
        grid=(n_heads,),
        in_specs=[
            pl.BlockSpec((n_seq, HEAD_DIM), lambda h: (0, h)),
            pl.BlockSpec((n_seq, HEAD_DIM), lambda h: (0, n_heads + h // group)),
            pl.BlockSpec((n_seq, HEAD_DIM), lambda h: (0, n_heads + n_kv + h // group)),
            tab, tab,
        ],
        out_specs=pl.BlockSpec((n_seq, HEAD_DIM), lambda h: (0, h)),
        out_shape=jax.ShapeDtypeStruct((n_seq, n_heads * HEAD_DIM), BF16),
        compiler_params=pltpu.CompilerParams(vmem_limit_bytes=40 << 20),
        cost_estimate=pl.CostEstimate(flops=8 << 30, bytes_accessed=6 << 20, transcendentals=3 << 20),
        name='attn_fwd',
    )(qkv, qkv, qkv, cos_t, sin_t)


def attn_bwd_kernel(q_ref, k_ref, v_ref, do_ref, cos_ref, sin_ref, dq_ref, dk_ref, dv_ref, bq_ref, bk_ref, bv_ref, dk_acc, dv_acc):
    step = pl.program_id(1)
    cos_t, sin_t = cos_ref[...], sin_ref[...]
    q_rot = rope(q_ref[...], cos_t, sin_t).astype(BF16)
    k_rot = rope(k_ref[...], cos_t, sin_t).astype(BF16)
    v_st = v_ref[...].astype(BF16)
    d_out = do_ref[...]
    scores = dot_nt(k_rot, q_rot) * SCALE
    keep = lax.broadcasted_iota(jnp.int32, scores.shape, 1) >= lax.broadcasted_iota(jnp.int32, scores.shape, 0)
    scores = jnp.where(keep, scores, -1e30)
    probs = jnp.exp(scores - jnp.max(scores, axis=0, keepdims=True))
    probs = probs * (1.0 / jnp.sum(probs, axis=0, keepdims=True))
    d_v = dot_nn(probs.astype(BF16), d_out)
    d_probs = dot_nt(v_st, d_out)
    d_sc = (probs * (d_probs - jnp.sum(probs * d_probs, axis=0, keepdims=True)) * SCALE).astype(BF16)
    d_k = dot_nn(d_sc, q_rot)
    d_q = dot_tn(d_sc, k_rot).astype(BF16).astype(F32)
    d_q = rope_t(d_q, cos_t, sin_t)
    dq_ref[...] = d_q.astype(BF16)
    bq_ref[...] = jnp.sum(d_q, axis=0, keepdims=True)

    @pl.when(step == 0)
    def _():
        dk_acc[...] = d_k
        dv_acc[...] = d_v

    @pl.when(step > 0)
    def _():
        dk_acc[...] += d_k
        dv_acc[...] += d_v

    @pl.when(step == pl.num_programs(1) - 1)
    def _():
        d_k_all = rope_t(dk_acc[...].astype(BF16).astype(F32), cos_t, sin_t)
        dk_ref[...] = d_k_all.astype(BF16)
        bk_ref[...] = jnp.sum(d_k_all, axis=0, keepdims=True)
        d_v_all = dv_acc[...].astype(BF16)
        dv_ref[...] = d_v_all
        bv_ref[...] = jnp.sum(d_v_all.astype(F32), axis=0, keepdims=True)


def attn_bwd(qkv, d_attn, cos_t, sin_t, n_heads, n_kv):
    n_seq = qkv.shape[0]
    group = n_heads // n_kv
    tab = pl.BlockSpec((n_seq, HEAD_DIM), lambda j, g: (0, 0))
    blk_h = pl.BlockSpec((n_seq, HEAD_DIM), lambda j, g: (0, j * group + g))
    blk_kv = pl.BlockSpec((n_seq, HEAD_DIM), lambda j, g: (0, j))
    vec_h = pl.BlockSpec((1, HEAD_DIM), lambda j, g: (0, j * group + g))
    vec_kv = pl.BlockSpec((1, HEAD_DIM), lambda j, g: (0, j))
    q_width, kv_width = n_heads * HEAD_DIM, n_kv * HEAD_DIM
    return pl.pallas_call(
        attn_bwd_kernel,
        grid=(n_kv, group),
        in_specs=[
            blk_h,
            pl.BlockSpec((n_seq, HEAD_DIM), lambda j, g: (0, n_heads + j)),
            pl.BlockSpec((n_seq, HEAD_DIM), lambda j, g: (0, n_heads + n_kv + j)),
            blk_h, tab, tab,
        ],
        out_specs=[blk_h, blk_kv, blk_kv, vec_h, vec_kv, vec_kv],
        out_shape=[
            jax.ShapeDtypeStruct((n_seq, q_width), BF16),
            jax.ShapeDtypeStruct((n_seq, kv_width), BF16),
            jax.ShapeDtypeStruct((n_seq, kv_width), BF16),
            jax.ShapeDtypeStruct((1, q_width), F32),
            jax.ShapeDtypeStruct((1, kv_width), F32),
            jax.ShapeDtypeStruct((1, kv_width), F32),
        ],
        scratch_shapes=[pltpu.VMEM((n_seq, HEAD_DIM), F32), pltpu.VMEM((n_seq, HEAD_DIM), F32)],
        compiler_params=pltpu.CompilerParams(vmem_limit_bytes=40 << 20),
        cost_estimate=pl.CostEstimate(flops=16 << 30, bytes_accessed=10 << 20, transcendentals=3 << 20),
        name='attn_bwd',
    )(qkv, qkv, qkv, d_attn, cos_t, sin_t)


GRAD_BLK = 256


def attn_grads_kernel(n_o, n_all, lhs_o_ref, lhs_h_ref, rhs_o_ref, rhs_h_ref, small_ref, out_ref):
    step = pl.program_id(0)

    @pl.when(step < n_o)
    def _():
        out_ref[...] = dot_nn(lhs_o_ref[...], rhs_o_ref[...])

    @pl.when(jnp.logical_and(step >= n_o, step < n_all))
    def _():
        out_ref[...] = dot_nn(lhs_h_ref[...], rhs_h_ref[...])

    @pl.when(step == n_all)
    def _():
        out_ref[...] = small_ref[...]


def attn_grads(lhs_o, rhs_o, lhs_h, rhs_h, small):
    width, n_seq = lhs_o.shape
    n_o, n_h = rhs_o.shape[1] // GRAD_BLK, rhs_h.shape[1] // GRAD_BLK
    n_all = n_o + n_h
    full = pl.BlockSpec((width, n_seq), lambda j: (0, 0))
    return pl.pallas_call(
        lambda *refs: attn_grads_kernel(n_o, n_all, *refs),
        grid=(n_all + 1,),
        in_specs=[
            full, full,
            pl.BlockSpec((n_seq, GRAD_BLK), lambda j: (0, jnp.minimum(j, n_o - 1))),
            pl.BlockSpec((n_seq, GRAD_BLK), lambda j: (0, jnp.clip(j - n_o, 0, n_h - 1))),
            pl.BlockSpec((width, GRAD_BLK), lambda j: (0, 0)),
        ],
        out_specs=pl.BlockSpec((width, GRAD_BLK), lambda j: (0, j)),
        out_shape=jax.ShapeDtypeStruct((width, (n_all + 1) * GRAD_BLK), F32),
        compiler_params=pltpu.CompilerParams(vmem_limit_bytes=40 << 20),
        cost_estimate=pl.CostEstimate(flops=12 << 30, bytes_accessed=32 << 20, transcendentals=0),
        name='attn_grads',
    )(lhs_o, lhs_h, rhs_o, rhs_h, small)


def norm_fwd(hidden, gain_vec):
    x_f32 = hidden.astype(F32)
    inv_rms = lax.rsqrt(jnp.mean(x_f32 * x_f32, axis=-1, keepdims=True) + NORM_EPS)
    return (x_f32 * inv_rms * gain_vec).astype(BF16), inv_rms


def norm_bwd(hidden, inv_rms, gain_vec, d_normed):
    unit_rows = hidden.astype(F32) * inv_rms
    d_gain = jnp.sum(d_normed * unit_rows, axis=0)
    d_unit = d_normed * gain_vec
    d_hidden = inv_rms * (d_unit - unit_rows * jnp.mean(d_unit * unit_rows, axis=-1, keepdims=True))
    return d_hidden, d_gain


def cut_kernel(blk, n_rank, gate_ref, up_ref, out_ref):
    for r in range(n_rank):
        for g, src in enumerate((gate_ref, up_ref)):
            out_ref[r, g, :, 0:blk] = src[:, r * blk:(r + 1) * blk]
            out_ref[r, g, :, blk:2 * blk] = src[:, (n_rank + r) * blk:(n_rank + r + 1) * blk]


def cut_columns(w_gate, w_up, blk):
    rows = w_gate.shape[0]
    return pl.pallas_call(
        lambda *refs: cut_kernel(blk, TP, *refs),
        out_shape=jax.ShapeDtypeStruct((TP, 2, rows, 2 * blk), BF16),
        in_specs=[pl.BlockSpec(memory_space=pltpu.VMEM)] * 2,
        out_specs=pl.BlockSpec(memory_space=pltpu.VMEM),
        compiler_params=pltpu.CompilerParams(vmem_limit_bytes=24 << 20),
        cost_estimate=pl.CostEstimate(flops=4 << 30, bytes_accessed=8 << 20, transcendentals=0),
        name='cut_columns',
    )(w_gate, w_up)


def join_kernel(blk, n_rank, src_ref, out_ref):
    for r in range(n_rank):
        out_ref[:, r * blk:(r + 1) * blk] = src_ref[r, :, 0:blk]
        out_ref[:, (n_rank + r) * blk:(n_rank + r + 1) * blk] = src_ref[r, :, blk:2 * blk]


def join_columns(parts, blk):
    rows = parts.shape[1]
    tile = 32
    return pl.pallas_call(
        lambda *refs: join_kernel(blk, TP, *refs),
        grid=(rows // tile,),
        out_shape=jax.ShapeDtypeStruct((rows, 2 * TP * blk), F32),
        in_specs=[pl.BlockSpec((TP, tile, 2 * blk), lambda i: (0, i, 0))],
        out_specs=pl.BlockSpec((tile, 2 * TP * blk), lambda i: (i, 0)),
        compiler_params=pltpu.CompilerParams(vmem_limit_bytes=24 << 20),
        cost_estimate=pl.CostEstimate(flops=4 << 30, bytes_accessed=8 << 20, transcendentals=0),
        name='join_columns',
    )(parts)


def add_kernel(a_ref, b_ref, out_ref):
    out_ref[...] = a_ref[...] + b_ref[...]


def add_rows(lhs, rhs):
    rows, cols = lhs.shape
    blk = pl.BlockSpec((rows // 4, cols), lambda i: (i, 0))
    return pl.pallas_call(
        add_kernel, grid=(4,), in_specs=[blk, blk], out_specs=blk,
        out_shape=jax.ShapeDtypeStruct((rows, cols), F32),
        compiler_params=pltpu.CompilerParams(vmem_limit_bytes=24 << 20),
        cost_estimate=pl.CostEstimate(flops=4 << 30, bytes_accessed=12 << 20, transcendentals=0),
        name='add_rows',
    )(lhs, rhs)


def scatter_kernel(cols, g_ref, out_ref, own, from_core, buf1, buf2, buf3, load_sem, send_sem, recv_sem):
    dev = lax.axis_index(AX)
    me = (dev // 8, (dev // 4) % 2, (dev // 2) % 2)
    core = dev % 2
    peer_core = dev + 1 - 2 * core
    peers = tuple(dev + step * (1 - 2 * pos) for step, pos in zip((8, 4, 2), me))
    barrier_sem = pltpu.get_barrier_semaphore()
    for peer in (peer_core,) + peers:
        pl.semaphore_signal(barrier_sem, inc=1, device_id=(peer,), device_id_type=pl.DeviceIdType.MESH)
    pl.semaphore_wait(barrier_sem, 4)
    orders = ((2, 1, 0), (1, 0, 2), (0, 2, 1))
    load = pltpu.make_async_copy(g_ref.at[:, :, :, core], own, load_sem)
    load.start()

    def pick(fixed):
        return tuple(fixed.get(d, slice(None)) for d in range(3))

    def remote(slot, src, dst, peer):
        copy = pltpu.make_async_remote_copy(
            src_ref=src, dst_ref=dst, send_sem=send_sem.at[slot], recv_sem=recv_sem.at[slot],
            device_id=(peer,), device_id_type=pl.DeviceIdType.MESH)
        copy.start()
        return copy

    def col(k):
        return pl.ds(k * cols, cols)

    core_copies = {}
    for half in range(2):
        for k, order in enumerate(orders):
            where = pick({order[0]: me[order[0]] if half else 1 - me[order[0]]})
            core_copies[half, k] = remote(
                half * 3 + k, g_ref.at[where + (1 - core, slice(None), col(k))],
                from_core.at[where + (slice(None), col(k))], peer_core)
    load.wait()

    def add(dst, src, count):
        def body(i, carry):
            a, b = i // 2, i % 2
            dst(a, b)[...] = dst(a, b)[...] + src(a, b)[...]
            return carry

        lax.fori_loop(0, count, body, 0)

    def at4(ref, k, order, first):
        def get(a, b):
            fixed = {order[0]: first, order[1]: a, order[2]: b}
            return ref.at[tuple(fixed[d] for d in range(3)) + (slice(None), col(k))]

        return get

    def at2(ref, k, order, second):
        def get(a, b):
            fixed = {order[0]: me[order[0]], order[1]: second, order[2]: b}
            return ref.at[tuple(fixed[d] for d in range(3)) + (slice(None), col(k))]

        return get

    stage1, stage2, stage3 = {}, {}, {}
    for k, order in enumerate(orders):
        core_copies[0, k].wait_recv()
        far = 1 - me[order[0]]
        add(at4(own, k, order, far), at4(from_core, k, order, far), 4)
    for k, order in enumerate(orders):
        for a in range(2):
            for b in range(2):
                fixed = {order[0]: 1 - me[order[0]], order[1]: a, order[2]: b}
                src = own.at[tuple(fixed[d] for d in range(3)) + (slice(None), col(k))]
                stage1[k, a, b] = remote(6 + k * 4 + a * 2 + b, src, buf1.at[k, a, b], peers[order[0]])
    for k, order in enumerate(orders):
        core_copies[1, k].wait_recv()
        near = me[order[0]]
        add(at4(own, k, order, near), at4(from_core, k, order, near), 4)
    for k, order in enumerate(orders):
        for a in range(2):
            for b in range(2):
                stage1[k, a, b].wait_recv()
        add(at4(own, k, order, me[order[0]]), lambda a, b, k=k: buf1.at[k, a, b], 4)
    for k, order in enumerate(orders):
        for b in range(2):
            src = at2(own, k, order, 1 - me[order[1]])(0, b)
            stage2[k, b] = remote(18 + k * 2 + b, src, buf2.at[k, b], peers[order[1]])
    for k, order in enumerate(orders):
        for b in range(2):
            stage2[k, b].wait_recv()
        add(at2(own, k, order, me[order[1]]), lambda a, b, k=k: buf2.at[k, b], 2)
    for k, order in enumerate(orders):
        src = at2(own, k, order, me[order[1]])(0, 1 - me[order[2]])
        stage3[k] = remote(24 + k, src, buf3.at[k], peers[order[2]])
    for k, order in enumerate(orders):
        stage3[k].wait_recv()
        out_ref[:, k * cols:(k + 1) * cols] = at2(own, k, order, me[order[1]])(0, me[order[2]])[...] + buf3[k]
    for copy in list(core_copies.values()) + list(stage1.values()) + list(stage2.values()) + list(stage3.values()):
        copy.wait_send()


def scatter_all(grads, rows):
    cols = grads.shape[1] // 3
    g6 = grads.reshape(2, 2, 2, 2, rows, 3 * cols)
    return pl.pallas_call(
        lambda *refs: scatter_kernel(cols, *refs),
        out_shape=jax.ShapeDtypeStruct((rows, 3 * cols), F32),
        in_specs=[pl.BlockSpec(memory_space=pl.ANY)],
        out_specs=pl.BlockSpec(memory_space=pltpu.VMEM),
        scratch_shapes=[
            pltpu.VMEM((2, 2, 2, rows, 3 * cols), F32),
            pltpu.VMEM((2, 2, 2, rows, 3 * cols), F32),
            pltpu.VMEM((3, 2, 2, rows, cols), F32),
            pltpu.VMEM((3, 2, rows, cols), F32),
            pltpu.VMEM((3, rows, cols), F32),
            pltpu.SemaphoreType.DMA,
            pltpu.SemaphoreType.DMA((27,)),
            pltpu.SemaphoreType.DMA((27,)),
        ],
        compiler_params=pltpu.CompilerParams(collective_id=0, has_side_effects=True, vmem_limit_bytes=52 << 20),
        cost_estimate=pl.CostEstimate(flops=60 << 30, bytes_accessed=64 << 20, transcendentals=0),
        name='scatter_all',
    )(g6)


def z_pair(arr):
    return lax.ppermute(arr, AX, Z_PERM)


barrier = lax.optimization_barrier


def group_gather(arr):
    return lax.all_gather(arr, AX, axis=0, tiled=True, axis_index_groups=GROUPS)


def group_scatter(arr):
    return lax.psum_scatter(arr, AX, scatter_dimension=0, tiled=True, axis_index_groups=GROUPS)


def xor_send(arr, step):
    return lax.ppermute(arr, AX, [(i, i ^ step) for i in range(N_DEV)])


def plane_gather(arr, rank):
    n_half = arr.shape[0] // CHUNKS
    via_x, via_y = xor_send(arr, 2), xor_send(arr, 4)
    halves = {0: (arr[:n_half], arr[n_half:]), 2: (via_x[:n_half], via_x[n_half:]), 4: (via_y[:n_half], via_y[n_half:])}
    halves[6] = (xor_send(halves[4][0], 2), xor_send(halves[2][1], 4))
    own_core, x_core, y_core = xor_send(arr, 1), xor_send(via_x, 1), xor_send(via_y, 1)
    for step, both in ((1, own_core), (3, x_core), (5, y_core)):
        halves[step] = (both[:n_half], both[n_half:])
    halves[7] = tuple(xor_send(part, 1) for part in halves[6])
    out = []
    for c in range(CHUNKS):
        buf = jnp.zeros((TP,) + halves[0][c].shape, BF16)
        for step in range(TP):
            buf = lax.dynamic_update_slice(buf, halves[step][c][None], (rank ^ step, 0, 0))
        out.append(buf.reshape(TP * n_half, arr.shape[1]))
    return out


def local_step(hidden, grad_out, positions, gain_attn, w_q, b_q, w_k, b_k, w_v, b_v, w_o, gain_mlp, w_gate, w_up, w_down):
    n_seq, width = hidden.shape[1], hidden.shape[2]
    rows = w_q.shape[0]
    q_width, kv_width = w_q.shape[1], w_k.shape[1]
    n_heads, n_kv = q_width // HEAD_DIM, kv_width // HEAD_DIM
    ff_blk = w_down.shape[0]
    ff_loc = 2 * ff_blk
    half = width // 2
    dev = lax.axis_index(AX)
    z_idx, rank = dev // TP, dev % TP
    z_zero = z_idx == 0
    hidden = hidden[0]
    grad_out = grad_out[0]

    kvb = jnp.concatenate([b_k, b_v, jnp.zeros((rows - 2 * b_k.shape[0],), BF16)])
    small = jnp.stack([gain_attn, b_q, gain_mlp, kvb], axis=1)
    small = jnp.pad(small, ((0, 0), (0, 124)))
    qkv_loc = jnp.concatenate([w_q, w_k, w_v, small], axis=1)
    qkv_full = lax.all_gather(qkv_loc, AX, axis=0, tiled=True)
    n_qkv = q_width + 2 * kv_width
    w_o_full = lax.all_gather(w_o, AX, axis=0, tiled=True)

    gu = cut_columns(w_gate, w_up, ff_blk)
    gu, hidden = barrier((gu, hidden))
    own_rows, other_rows = [], []
    for g in range(2):
        buf = jnp.zeros((TP, rows, ff_loc), BF16)
        for d in range(TP):
            piece = lax.dynamic_slice(gu, (rank ^ d, g, 0, 0), (1, 1, rows, ff_loc))[:, 0]
            if d:
                piece = lax.ppermute(piece, AX, [(i, i ^ d) for i in range(N_DEV)])
            buf = lax.dynamic_update_slice(buf, piece, (rank ^ d, 0, 0))
        buf = buf.reshape(half, ff_loc)
        own_rows.append(buf)
        other_rows.append(z_pair(buf))
    down_other = z_pair(w_down)

    w_qkv = qkv_full[:, :n_qkv]
    small_t = qkv_full[:, n_qkv:n_qkv + 4].T.astype(F32)
    gain_a, bias_q, gain_m = small_t[0], small_t[1], small_t[2]
    kvb_full = small_t[3].reshape(N_DEV, rows)
    n_b = b_k.shape[0]
    bias = jnp.concatenate([bias_q, kvb_full[:, :n_b].reshape(kv_width), kvb_full[:, n_b:2 * n_b].reshape(kv_width)])
    cos_t, sin_t = rope_tables(positions[0])
    normed_attn, inv_attn = norm_fwd(hidden, gain_a)
    qkv = dot('sd,de->se', normed_attn, w_qkv) + bias
    attn_out = attn_fwd(qkv, cos_t, sin_t, n_heads, n_kv)
    resid_mid = (hidden.astype(F32) + dot('se,ed->sd', attn_out, w_o_full)).astype(BF16)
    normed_mlp, inv_mlp = norm_fwd(resid_mid, gain_m)
    grad_late, _ = barrier((grad_out, resid_mid))
    go_all = plane_gather(grad_late, rank)
    n_ch = n_seq // CHUNKS
    h_all = [group_gather(normed_mlp[c * n_ch:(c + 1) * n_ch]) for c in range(CHUNKS)]

    def z_order(own, other):
        return jnp.concatenate([jnp.where(z_zero, own, other), jnp.where(z_zero, other, own)], axis=0)

    w_g, w_u = z_order(own_rows[0], other_rows[0]), z_order(own_rows[1], other_rows[1])

    pre = []
    for c in range(CHUNKS):
        gate_pre = dot('sd,df->sf', h_all[c], w_g)
        up_proj = dot('sd,df->sf', h_all[c], w_u)
        pre.append((gate_pre, up_proj))
    down_late, _ = barrier((down_other, pre[0][0]))
    w_d = z_order(w_down, down_late)
    acts, d_gates, d_ups, dn_sums = [], [], [], []
    gate_pre, up_proj = pre[0]
    act_first = (jax.nn.silu(gate_pre) * up_proj).astype(BF16)
    out_first = dot('sf,fd->sd', act_first, w_d)
    out_first, go_all[0] = barrier((out_first, go_all[0]))
    out_sums = [group_scatter(out_first)]
    for c in range(CHUNKS):
        gate_pre, up_proj = pre[c]
        act = act_first if c == 0 else (jax.nn.silu(gate_pre) * up_proj).astype(BF16)
        d_act = dot('sd,fd->sf', go_all[c], w_d).astype(BF16).astype(F32)
        gate_sig = jax.nn.sigmoid(gate_pre)
        d_gate = (d_act * up_proj * gate_sig * (1.0 + gate_pre * (1.0 - gate_sig))).astype(BF16)
        d_up = (d_act * gate_pre * gate_sig).astype(BF16)
        dn_part = dot('sf,df->sd', d_gate, w_g) + dot('sf,df->sd', d_up, w_u)
        dn_sums.append(group_scatter(dn_part))
        acts.append(act)
        d_gates.append(d_gate)
        d_ups.append(d_up)
    dn_part, acts, d_gates, d_ups, h_all = barrier((dn_part, acts, d_gates, d_ups, h_all))

    def token_dot(eq_form, lhs_list, rhs_list):
        total = dot(eq_form, lhs_list[0], rhs_list[0])
        for lhs, rhs in zip(lhs_list[1:], rhs_list[1:]):
            total = total + dot(eq_form, lhs, rhs)
        return total

    h_send = [lax.dynamic_slice_in_dim(h, (1 - z_idx) * half, half, axis=1) for h in h_all]
    h_keep = [lax.dynamic_slice_in_dim(h, z_idx * half, half, axis=1) for h in h_all]
    gg_send = token_dot('sd,sf->df', h_send, d_gates)
    gu_send = token_dot('sd,sf->df', h_send, d_ups)
    d_wd = token_dot('sf,sd->fd', acts, go_all)
    wd_send = lax.dynamic_slice_in_dim(d_wd, (1 - z_idx) * ff_blk, ff_blk, axis=0)
    wd_keep = lax.dynamic_slice_in_dim(d_wd, z_idx * ff_blk, ff_blk, axis=0)
    gg_recv, gu_recv, wd_recv = z_pair(gg_send), z_pair(gu_send), z_pair(wd_send)
    gg_keep = token_dot('sd,sf->df', h_keep, d_gates)
    gu_keep = token_dot('sd,sf->df', h_keep, d_ups)
    out_part = [dot('sf,fd->sd', act, w_d) for act in acts[1:]]
    gu_sum = add_rows(gu_keep, gu_recv)
    dn_sums, gg_keep, gu_sum, out_part, wd_keep = barrier((dn_sums, gg_keep, gu_sum, out_part, wd_keep))
    d_normed_mlp = jnp.concatenate(dn_sums, axis=0).astype(BF16).astype(F32)
    out_sum = jnp.concatenate(out_sums + [group_scatter(part) for part in out_part], axis=0)

    def back_rows(grad):
        grad = lax.all_to_all(grad.reshape(TP, rows, ff_loc), AX, 0, 0, axis_index_groups=GROUPS, tiled=True)
        return grad

    up_parts = back_rows(gu_sum)
    g_w_up = join_columns(up_parts, ff_blk)

    d_resid_norm, d_gain_m = norm_bwd(resid_mid, inv_mlp, gain_m, d_normed_mlp)
    d_resid = (grad_out.astype(F32) + d_resid_norm).astype(BF16)
    d_attn = dot('sd,ed->se', d_resid, w_o_full).astype(BF16)
    d_q, d_k, d_v, d_b_q, d_b_k, d_b_v = attn_bwd(qkv, d_attn, cos_t, sin_t, n_heads, n_kv)
    gg_keep, _, _ = barrier((gg_keep, d_b_k, up_parts))
    g_w_gate = join_columns(back_rows(add_rows(gg_keep, gg_recv)), ff_blk)
    d_qkv = jnp.concatenate([d_q, d_k, d_v], axis=1)
    d_normed_attn = dot('se,de->sd', d_qkv, w_qkv).astype(BF16).astype(F32)
    d_hidden_norm, d_gain_a = norm_bwd(hidden, inv_attn, gain_a, d_normed_attn)
    grad_hidden = (d_resid.astype(F32) + d_hidden_norm).astype(BF16)

    d_kvb = jnp.concatenate([d_b_k.reshape(N_DEV, n_b), d_b_v.reshape(N_DEV, n_b), jnp.zeros((N_DEV, rows - 2 * n_b), F32)], axis=1)
    d_small = jnp.stack([d_gain_a, d_b_q[0], d_gain_m, d_kvb.reshape(width)], axis=1)
    d_small = jnp.pad(d_small, ((0, 0), (0, GRAD_BLK - 4)))
    grads = attn_grads(attn_out.T, d_resid, normed_attn.T, d_qkv, d_small)
    grads = scatter_all(grads, rows)
    out_sum, wd_keep, grads = barrier((out_sum, wd_keep, grads))
    g_w_down = wd_keep + wd_recv
    layer_out = (resid_mid.astype(F32) + out_sum).astype(BF16)
    g_w_o, g_qkv = grads[:, :width], grads[:, width:]
    g_w_q = g_qkv[:, :q_width]
    g_w_k = g_qkv[:, q_width:q_width + kv_width]
    g_w_v = g_qkv[:, q_width + kv_width:n_qkv]
    g_small = g_qkv[:, n_qkv:n_qkv + 4].T
    g_kvb = g_small[3]
    return (layer_out[None], grad_hidden[None], g_small[0], g_w_q, g_small[1], g_w_k, g_kvb[:n_b], g_w_v, g_kvb[n_b:2 * n_b],
            g_w_o, g_small[2], g_w_gate, g_w_up, g_w_down)


def solution(mesh):
    act_spec = P(AX, None, None)
    mat_spec = P(AX, None)
    vec_spec = P(AX)
    param_specs = (vec_spec, mat_spec, vec_spec, mat_spec, vec_spec, mat_spec, vec_spec, mat_spec, vec_spec, mat_spec, mat_spec, mat_spec)
    in_specs_all = (act_spec, act_spec, mat_spec) + param_specs
    out_specs_all = (act_spec, act_spec) + param_specs

    return jax.shard_map(local_step, mesh=mesh, in_specs=in_specs_all, out_specs=out_specs_all, check_vma=False)
```
